256 devices in a mesh: row: 16 (over x_hi, z), col: 8 (over x_lo, y), rep: 2 (over core).
Axes of the slice: x: 4 (x_hi: 2, x_lo: 2; x = x_hi * 2 + x_lo), y: 4, z: 8, core: 2. Of those that a mesh axis runs over, the one named last changes fastest.
Arguments:
- matrix: float32 [16384, 16384], P('row', 'col'), may hold values from -0.125 to 0.125
- vectors: float32 [64, 16384], P('rep', 'row'), may hold values from -0.3 to 0.3
Outputs:
- result: float32 [64, 16384], P('rep', 'row')
The draws below stay inside these ranges and needn't reach their ends.
All inputs are finite; a program needn't handle non-finite values.
Results may differ from the reference program's by a relative error of at most 0.00011.
Values sent between devices are 32-bit elements; how exact they have to be, the bound alone decides.
No kernel may reach another device: no remote copies, remote signals or barrier semaphores. Data moves between devices by JAX's collectives and lax.ppermute only.
A program may use at most 64 MiB of HBM per device.

```python
import jax
import jax.numpy as jnp
from jax import lax

N = 16384
COLS = 64
TERMS = 6
STEPS = 1


def block_scale(rng, dims, split, smallest, largest):
    factor_of = 1.0
    for position, blocks in split:
        steps = jax.random.uniform(jax.random.fold_in(jax.random.fold_in(rng, 6), position), (blocks,), jnp.float32, smallest / len(split), largest / len(split))
        factor_of = factor_of * jnp.repeat(jnp.exp(steps), dims[position] // blocks).reshape((-1,) + (1,) * (len(dims) - 1 - position))
    return factor_of


def gaussian(stream_key, shape, deviation, limit, pieces=(), dtype=jnp.bfloat16):
    factor_of = block_scale(stream_key, shape, pieces, -0.22, 0.18) if pieces else 1.0
    entries = jax.random.normal(stream_key, shape, jnp.float32) * deviation * factor_of
    return jnp.minimum(jnp.maximum(entries, -limit), limit).astype(dtype)


def setup_inputs(seed: int = 0) -> dict:
    key_list = jax.random.split(jax.random.key(seed), 3)
    matrix = gaussian(key_list[0], (N, N), (N // 7) ** -0.5, 0.125, ((0, 16), (1, 8)), jnp.float32)
    vectors = gaussian(key_list[1], (COLS, N), 0.05, 0.3, ((0, 2), (1, 16)), jnp.float32)
    return {"matrix": matrix, "vectors": vectors}


def reference(matrix, vectors):
    current = vectors
    for section in range(STEPS):
        summand = current
        running = current
        for degree in range(1, TERMS + 1):
            product = lax.dot_general(summand, matrix, (((1,), (1,)), ((), ())), precision=lax.Precision.HIGHEST, preferred_element_type=jnp.float32)
            summand = product / float(degree * STEPS)
            running = running + summand
        current = running
    return current
```

```python
import functools

import jax
import jax.numpy as jnp
from jax import lax
from jax.experimental import pallas as pl
from jax.experimental.pallas import tpu as pltpu
from jax.sharding import Mesh, PartitionSpec as P

TERMS = 6
STEPS = 1

ROW = ("xh", "zh", "zl")
COL = ("xl", "y")
SIZES = {"xh": 2, "zh": 4, "zl": 2, "xl": 2, "y": 4, "rep": 2}


def owner_moves():
    def place(xh, zh, zl, xl, y):
        return (((xh * 4 + zh) * 2 + zl) * 2 + xl) * 4 + y

    return [
        (place(xh, zh, zl, xl, y), place(xl, (y + 2) % 4, zl, xh, zh))
        for xh in range(2)
        for zh in range(4)
        for zl in range(2)
        for xl in range(2)
        for y in range(4)
    ]


def split(value):
    high = value.astype(jnp.bfloat16)
    low = (value - high.astype(jnp.float32)).astype(jnp.bfloat16)
    return high, low


def prepare_kernel(a_ref, high_ref, low_ref, held, sems):
    blocks = held.shape[0]
    width = held.shape[2]

    def copy(block):
        return pltpu.make_async_copy(
            a_ref.at[:, pl.ds(pl.multiple_of(block * width, width), width)], held.at[block], sems.at[block]
        )

    for block in range(blocks):
        copy(block).start()

    def step(block, carry):
        copy(block).wait()
        high, low = split(held[block].T)
        rows = pl.ds(pl.multiple_of(block * width, width), width)
        high_ref[rows, :] = high
        low_ref[rows, :] = low
        return carry

    lax.fori_loop(0, blocks, step, 0)


def prepare(matrix):
    rows, columns = matrix.shape
    width = 256
    half = pltpu.VMEM((columns, rows), jnp.bfloat16)
    return pl.pallas_call(
        prepare_kernel,
        out_shape=(half, half),
        in_specs=[pl.BlockSpec(memory_space=pltpu.HBM)],
        out_specs=(pl.BlockSpec(memory_space=pltpu.VMEM),) * 2,
        scratch_shapes=[
            pltpu.VMEM((columns // width, rows, width), jnp.float32),
            pltpu.SemaphoreType.DMA((columns // width,)),
        ],
        cost_estimate=pl.CostEstimate(flops=4_000_000_000, bytes_accessed=8 << 20, transcendentals=0),
        compiler_params=pltpu.CompilerParams(vmem_limit_bytes=24 << 20),
    )(pltpu.with_memory_space_constraint(matrix, pltpu.HBM))


def product_tiles(x_ref, high_ref, low_ref, tile):
    pieces = [split(x_ref[piece]) for piece in range(x_ref.shape[0])]
    x_high = jnp.concatenate([high for high, _ in pieces], axis=1)
    x_low = jnp.concatenate([low for _, low in pieces], axis=1)
    both = jnp.concatenate([x_high, x_low], axis=0)
    vectors = x_high.shape[0]
    for start in range(0, high_ref.shape[1], tile):
        columns = slice(start, start + tile)
        first = jnp.dot(both, high_ref[:, columns], preferred_element_type=jnp.float32)
        second = jnp.dot(x_high, low_ref[:, columns], preferred_element_type=jnp.float32)
        yield start, first[:vectors] + (first[vectors:] + second)


def product_kernel(x_ref, high_ref, low_ref, out_ref):
    width = out_ref.shape[2]
    for start, total in product_tiles(x_ref, high_ref, low_ref, 256):
        side, within = divmod(start, width)
        for copy in range(4):
            out_ref[side * 4 + copy, :, within : within + 256] = total


def last_kernel(scale, x_ref, high_ref, low_ref, running_ref, out_ref):
    width = running_ref.shape[1]
    mine = lax.axis_index("xl")
    first = lax.axis_index("y") == 0
    for start, total in product_tiles(x_ref, high_ref, low_ref, 256):
        side, within = divmod(start, width)
        running = running_ref[:, within : within + 256]
        adds = jnp.logical_and(first, mine == side)
        total = total / scale + jnp.where(adds, running, jnp.zeros_like(running))
        for copy in range(8):
            out_ref[copy, :, start : start + 256] = total


def product(operand, halves, running=None, scale=None):
    vectors = operand.shape[1]
    rows = halves[0].shape[1]
    last = running is not None
    vmem = pl.BlockSpec(memory_space=pltpu.VMEM)
    operands = (operand, *halves) + ((running,) if last else ())
    return pl.pallas_call(
        functools.partial(last_kernel, scale) if last else product_kernel,
        out_shape=jax.ShapeDtypeStruct((8, vectors, rows if last else rows // 2), jnp.float32),
        in_specs=[vmem] * len(operands),
        out_specs=vmem,
        cost_estimate=pl.CostEstimate(flops=400_000_000, bytes_accessed=8 << 20, transcendentals=0),
        compiler_params=pltpu.CompilerParams(vmem_limit_bytes=8 << 20),
    )(*operands)


def combine_kernel(scale, parts_ref, running_ref, summand_ref, total_ref):
    summand = parts_ref[0]
    for part in range(1, parts_ref.shape[0]):
        summand = summand + parts_ref[part]
    summand = summand / scale
    summand_ref[...] = summand
    total_ref[...] = running_ref[...] + summand


def combine(parts, running, scale):
    vmem = pl.BlockSpec(memory_space=pltpu.VMEM)
    out = jax.ShapeDtypeStruct(running.shape, jnp.float32)
    return pl.pallas_call(
        functools.partial(combine_kernel, scale),
        out_shape=(out, out),
        in_specs=[vmem, vmem],
        out_specs=(vmem, vmem),
        cost_estimate=pl.CostEstimate(flops=1_000_000, bytes_accessed=1 << 19, transcendentals=0),
        compiler_params=pltpu.CompilerParams(vmem_limit_bytes=2 << 20),
    )(parts, running)


def exchange(value, axes):
    return lax.all_to_all(value, axes, 0, 0, tiled=True)


def move(piece):
    return lax.ppermute(piece, ROW + COL, owner_moves())


def gather(moved):
    return exchange(jnp.broadcast_to(moved[None], (4, *moved.shape)), ("zl", "xh"))


def local(matrix, vectors):
    half = vectors.shape[1] // 2
    running = jnp.where(lax.axis_index("xl") == 0, vectors[:, :half], vectors[:, half:])
    moved = move(running)
    halves = prepare(matrix)
    moved, halves = lax.optimization_barrier((moved, halves))
    for degree in range(1, TERMS):
        parts = exchange(product(gather(moved), halves), COL)
        summand, running = combine(parts, running, float(degree * STEPS))
        moved = move(summand)
    parts = exchange(product(gather(moved), halves, running, float(TERMS * STEPS)), COL)
    return functools.reduce(jnp.add, [parts[part] for part in range(8)])


def solution(mesh):
    fine = Mesh(mesh.devices.reshape(tuple(SIZES.values())), tuple(SIZES))
    placed = (P(ROW, COL), P("rep", ROW))
    return jax.shard_map(local, mesh=fine, in_specs=placed, out_specs=P("rep", ROW), check_vma=False)
```

```python
import functools

import jax
import jax.numpy as jnp
from jax import lax
from jax.experimental import pallas as pl
from jax.experimental.pallas import tpu as pltpu
from jax.sharding import Mesh, PartitionSpec as P

TERMS = 6
STEPS = 1

ROW = ("xh", "zh", "zl")
COL = ("xl", "y")
SIZES = {"xh": 2, "zh": 4, "zl": 2, "xl": 2, "y": 4, "rep": 2}


def owner_moves():
    def place(xh, zh, zl, xl, y):
        return (((xh * 4 + zh) * 2 + zl) * 2 + xl) * 4 + y

    return [
        (place(xh, zh, zl, xl, y), place(xl, (y + 2) % 4, zl, xh, zh))
        for xh in range(2)
        for zh in range(4)
        for zl in range(2)
        for xl in range(2)
        for y in range(4)
    ]


def split(value):
    high = value.astype(jnp.bfloat16)
    low = (value - high.astype(jnp.float32)).astype(jnp.bfloat16)
    return high, low


def prepare_kernel(a_ref, high_ref, low_ref, held, sems):
    blocks = held.shape[0]
    width = held.shape[2]

    def copy(block):
        return pltpu.make_async_copy(
            a_ref.at[:, pl.ds(pl.multiple_of(block * width, width), width)], held.at[block], sems.at[block]
        )

    for block in range(blocks):
        copy(block).start()

    def step(block, carry):
        copy(block).wait()
        high, low = split(held[block].T)
        rows = pl.ds(pl.multiple_of(block * width, width), width)
        high_ref[rows, :] = high
        low_ref[rows, :] = low
        return carry

    lax.fori_loop(0, blocks, step, 0)


def prepare(matrix):
    rows, columns = matrix.shape
    width = 256
    half = pltpu.VMEM((columns, rows), jnp.bfloat16)
    return pl.pallas_call(
        prepare_kernel,
        out_shape=(half, half),
        in_specs=[pl.BlockSpec(memory_space=pltpu.HBM)],
        out_specs=(pl.BlockSpec(memory_space=pltpu.VMEM),) * 2,
        scratch_shapes=[
            pltpu.VMEM((columns // width, rows, width), jnp.float32),
            pltpu.SemaphoreType.DMA((columns // width,)),
        ],
        cost_estimate=pl.CostEstimate(flops=4_000_000_000, bytes_accessed=8 << 20, transcendentals=0),
        compiler_params=pltpu.CompilerParams(vmem_limit_bytes=24 << 20),
    )(pltpu.with_memory_space_constraint(matrix, pltpu.HBM))


def product_tiles(x_ref, high_ref, low_ref, tile):
    pieces = [split(x_ref[piece]) for piece in range(x_ref.shape[0])]
    x_high = jnp.concatenate([high for high, _ in pieces], axis=1)
    x_low = jnp.concatenate([low for _, low in pieces], axis=1)
    both = jnp.concatenate([x_high, x_low], axis=0)
    vectors = x_high.shape[0]
    for start in range(0, high_ref.shape[1], tile):
        columns = slice(start, start + tile)
        first = jnp.dot(both, high_ref[:, columns], preferred_element_type=jnp.float32)
        second = jnp.dot(x_high, low_ref[:, columns], preferred_element_type=jnp.float32)
        yield start, first[:vectors] + (first[vectors:] + second)


def product_kernel(x_ref, high_ref, low_ref, out_ref):
    width = out_ref.shape[2]
    for start, total in product_tiles(x_ref, high_ref, low_ref, 256):
        side, within = divmod(start, width)
        for copy in range(4):
            out_ref[side * 4 + copy, :, within : within + 256] = total


def last_kernel(scale, x_ref, high_ref, low_ref, running_ref, out_ref):
    width = running_ref.shape[1]
    mine = lax.axis_index("xl")
    first = lax.axis_index("y") == 0
    for start, total in product_tiles(x_ref, high_ref, low_ref, 256):
        side, within = divmod(start, width)
        running = running_ref[:, within : within + 256]
        adds = jnp.logical_and(first, mine == side)
        total = total / scale + jnp.where(adds, running, jnp.zeros_like(running))
        for copy in range(8):
            out_ref[copy, :, start : start + 256] = total


def product(operand, halves, running=None, scale=None):
    vectors = operand.shape[1]
    rows = halves[0].shape[1]
    last = running is not None
    vmem = pl.BlockSpec(memory_space=pltpu.VMEM)
    operands = (operand, *halves) + ((running,) if last else ())
    return pl.pallas_call(
        functools.partial(last_kernel, scale) if last else product_kernel,
        out_shape=jax.ShapeDtypeStruct((8, vectors, rows if last else rows // 2), jnp.float32),
        in_specs=[vmem] * len(operands),
        out_specs=vmem,
        cost_estimate=pl.CostEstimate(flops=400_000_000, bytes_accessed=8 << 20, transcendentals=0),
        compiler_params=pltpu.CompilerParams(vmem_limit_bytes=8 << 20),
    )(*operands)


def combine_kernel(scale, parts_ref, running_ref, summand_ref, total_ref):
    summand = parts_ref[0]
    for part in range(1, parts_ref.shape[0]):
        summand = summand + parts_ref[part]
    summand = summand / scale
    summand_ref[...] = summand
    total_ref[...] = running_ref[...] + summand


def combine(parts, running, scale):
    vmem = pl.BlockSpec(memory_space=pltpu.VMEM)
    out = jax.ShapeDtypeStruct(running.shape, jnp.float32)
    return pl.pallas_call(
        functools.partial(combine_kernel, scale),
        out_shape=(out, out),
        in_specs=[vmem, vmem],
        out_specs=(vmem, vmem),
        cost_estimate=pl.CostEstimate(flops=1_000_000, bytes_accessed=1 << 19, transcendentals=0),
        compiler_params=pltpu.CompilerParams(vmem_limit_bytes=2 << 20),
    )(parts, running)


def exchange(value, axes):
    return lax.all_to_all(value, axes, 0, 0, tiled=True)


def move(piece):
    return lax.ppermute(piece, ROW + COL, owner_moves())


def gather(moved):
    return exchange(jnp.broadcast_to(moved[None], (4, *moved.shape)), ("zl", "xh"))


def series(matrix, vectors):
    half = vectors.shape[1] // 2
    running = jnp.where(lax.axis_index("xl") == 0, vectors[:, :half], vectors[:, half:])
    moved = move(running)
    halves = prepare(matrix)
    moved, halves = lax.optimization_barrier((moved, halves))
    for degree in range(1, TERMS):
        parts = exchange(product(gather(moved), halves), COL)
        summand, running = combine(parts, running, float(degree * STEPS))
        moved = move(summand)
    parts = exchange(product(gather(moved), halves, running, float(TERMS * STEPS)), COL)
    return functools.reduce(jnp.add, [parts[part] for part in range(8)])


def local(matrix, vectors):
    count = vectors.shape[0]
    other = lax.ppermute(vectors, "rep", [(0, 1)])
    both = jnp.concatenate([other, vectors], axis=0)
    result = lax.cond(lax.axis_index("rep") == 1, series, lambda matrix, both: both, matrix, both)
    back = lax.ppermute(result[:count], "rep", [(1, 0)])
    return jnp.where(lax.axis_index("rep") == 1, result[count:], back)


def solution(mesh):
    fine = Mesh(mesh.devices.reshape(tuple(SIZES.values())), tuple(SIZES))
    placed = (P(ROW, COL), P("rep", ROW))
    return jax.shard_map(local, mesh=fine, in_specs=placed, out_specs=P("rep", ROW), check_vma=False)
```

```python
import functools

import jax
import jax.numpy as jnp
from jax import lax
from jax.experimental import pallas as pl
from jax.experimental.pallas import tpu as pltpu
from jax.sharding import Mesh, PartitionSpec as P

TERMS = 6
STEPS = 1

ROW = ("xh", "zh", "zl")
COL = ("xl", "y")
SIZES = {"xh": 2, "zh": 4, "zl": 2, "xl": 2, "y": 4, "rep": 2}
PLACES = [
    (xh, zh, zl, xl, y)
    for xh in range(2)
    for zh in range(4)
    for zl in range(2)
    for xl in range(2)
    for y in range(4)
]
FAR = 2


def index(xh, zh, zl, xl, y):
    return (((xh * 4 + zh) * 2 + zl) * 2 + xl) * 4 + y


def owner_moves():
    return [
        (index(xh, zh, zl, xl, y), index(xl, (y + FAR) % 4, zl ^ int(y == zh), xh, zh))
        for xh, zh, zl, xl, y in PLACES
    ]


def neighbour_moves():
    return [(index(xh, zh, zl, xl, y), index(xh, zh, 1 - zl, xl, y)) for xh, zh, zl, xl, y in PLACES]


def split(value):
    high = value.astype(jnp.bfloat16)
    low = (value - high.astype(jnp.float32)).astype(jnp.bfloat16)
    return high, low


def prepare_kernel(a_ref, high_ref, low_ref, held, sems):
    blocks = held.shape[0]
    width = held.shape[2]
    swapped = lax.rem(lax.axis_index("y") + FAR, 4) == lax.axis_index("zh")
    mine = lax.axis_index("zl") ^ swapped.astype(jnp.int32)

    def copy(block):
        column = pl.multiple_of(block * width, width)
        return pltpu.make_async_copy(a_ref.at[:, pl.ds(column, width)], held.at[block], sems.at[block])

    for block in range(blocks):
        copy(block).start()

    def step(block, carry):
        copy(block).wait()
        high, low = split(held[block].T)
        place = lax.rem(block + mine * (blocks // 2), blocks)
        rows = pl.ds(pl.multiple_of(place * width, width), width)
        high_ref[rows, :] = high
        low_ref[rows, :] = low
        return carry

    lax.fori_loop(0, blocks, step, 0)


def prepare(matrix):
    rows, columns = matrix.shape
    width = 256
    half = pltpu.VMEM((columns, rows), jnp.bfloat16)
    return pl.pallas_call(
        prepare_kernel,
        out_shape=(half, half),
        in_specs=[pl.BlockSpec(memory_space=pltpu.HBM)],
        out_specs=(pl.BlockSpec(memory_space=pltpu.VMEM),) * 2,
        scratch_shapes=[
            pltpu.VMEM((columns // width, rows, width), jnp.float32),
            pltpu.SemaphoreType.DMA((columns // width,)),
        ],
        cost_estimate=pl.CostEstimate(flops=4_000_000_000, bytes_accessed=8 << 20, transcendentals=0),
        compiler_params=pltpu.CompilerParams(vmem_limit_bytes=24 << 20),
    )(pltpu.with_memory_space_constraint(matrix, pltpu.HBM))


def half_product(x_ref, high_ref, low_ref, which):
    x_high, x_low = split(x_ref[...])
    both = jnp.concatenate([x_high, x_low], axis=0)
    vectors, depth = x_high.shape
    rows = slice(which * depth, (which + 1) * depth)
    for start in range(0, high_ref.shape[1], 256):
        columns = slice(start, start + 256)
        first = jnp.dot(both, high_ref[rows, columns], preferred_element_type=jnp.float32)
        second = jnp.dot(x_high, low_ref[rows, columns], preferred_element_type=jnp.float32)
        yield columns, first[:vectors] + (first[vectors:] + second)


def first_kernel(x_ref, high_ref, low_ref, out_ref):
    for columns, total in half_product(x_ref, high_ref, low_ref, 0):
        out_ref[:, columns] = total


def second_kernel(x_ref, high_ref, low_ref, before_ref, out_ref):
    for columns, total in half_product(x_ref, high_ref, low_ref, 1):
        total = before_ref[:, columns] + total
        for copy in range(out_ref.shape[0]):
            out_ref[copy, :, columns] = total


def combine_kernel(scale, parts_ref, running_ref, summand_ref, total_ref):
    summand = parts_ref[0]
    for part in range(1, parts_ref.shape[0]):
        summand = summand + parts_ref[part]
    summand = summand / scale
    summand_ref[...] = summand
    total_ref[...] = running_ref[...] + summand


def call(kernel, out, flops, limit, *operands):
    vmem = pl.BlockSpec(memory_space=pltpu.VMEM)
    shapes = jax.tree.map(lambda shape: jax.ShapeDtypeStruct(shape, jnp.float32), out, is_leaf=lambda o: isinstance(o[0], int))
    return pl.pallas_call(
        kernel,
        out_shape=shapes,
        in_specs=[vmem] * len(operands),
        out_specs=jax.tree.map(lambda _: vmem, shapes),
        cost_estimate=pl.CostEstimate(flops=flops, bytes_accessed=4 << 20, transcendentals=0),
        compiler_params=pltpu.CompilerParams(vmem_limit_bytes=limit),
    )(*operands)


def product(block, halves):
    shape = block.shape
    other = lax.ppermute(block, ROW + COL, neighbour_moves())
    before = call(first_kernel, shape, 200_000_000, 4 << 20, block, *halves)
    return call(second_kernel, (8, *shape), 200_000_000, 4 << 20, other, *halves, before)


def local(matrix, vectors):
    shape = vectors.shape
    block = lax.ppermute(vectors, ROW + COL, owner_moves())
    halves = prepare(matrix)
    block, halves = lax.optimization_barrier((block, halves))
    running = vectors
    for degree in range(1, TERMS + 1):
        parts = lax.all_to_all(product(block, halves), COL, 0, 0, tiled=True)
        kernel = functools.partial(combine_kernel, float(degree * STEPS))
        summand, running = call(kernel, (shape, shape), 1_000_000, 2 << 20, parts, running)
        if degree < TERMS:
            block = lax.ppermute(summand, ROW + COL, owner_moves())
    return running


def solution(mesh):
    fine = Mesh(mesh.devices.reshape(tuple(SIZES.values())), tuple(SIZES))
    placed = (P(ROW, COL), P("rep", ROW))
    return jax.shard_map(local, mesh=fine, in_specs=placed, out_specs=P("rep", ROW), check_vma=False)
```

```python
import functools

import jax
import jax.numpy as jnp
from jax import lax
from jax.experimental import pallas as pl
from jax.experimental.pallas import tpu as pltpu
from jax.sharding import Mesh, PartitionSpec as P

TERMS = 6
STEPS = 1

ROW = ("xh", "zh", "zl")
COL = ("xl", "y")
SIZES = {"xh": 2, "zh": 4, "zl": 2, "xl": 2, "y": 4, "rep": 2}
PLACES = [
    (xh, zh, zl, xl, y)
    for xh in range(2)
    for zh in range(4)
    for zl in range(2)
    for xl in range(2)
    for y in range(4)
]
FAR = 2


def index(xh, zh, zl, xl, y):
    return (((xh * 4 + zh) * 2 + zl) * 2 + xl) * 4 + y


def owner_moves():
    def across(zh, y):
        return y if (y - zh) % 2 else (y + FAR) % 4

    return [
        (index(xh, zh, zl, xl, y), index(xl, across(zh, y), zl ^ int(y == zh), xh, zh))
        for xh, zh, zl, xl, y in PLACES
    ]


def neighbour_moves():
    return [(index(xh, zh, zl, xl, y), index(xh, zh, 1 - zl, xl, y)) for xh, zh, zl, xl, y in PLACES]


def split(value):
    high = value.astype(jnp.bfloat16)
    low = (value - high.astype(jnp.float32)).astype(jnp.bfloat16)
    return high, low


def prepare_kernel(a_ref, high_ref, low_ref, held, sems):
    blocks = held.shape[0]
    width = held.shape[2]
    swapped = lax.rem(lax.axis_index("y") + FAR, 4) == lax.axis_index("zh")
    mine = lax.axis_index("zl") ^ swapped.astype(jnp.int32)

    def copy(block):
        column = pl.multiple_of(block * width, width)
        return pltpu.make_async_copy(a_ref.at[:, pl.ds(column, width)], held.at[block], sems.at[block])

    for block in range(blocks):
        copy(block).start()

    def step(block, carry):
        copy(block).wait()
        high, low = split(held[block].T)
        place = lax.rem(block + mine * (blocks // 2), blocks)
        rows = pl.ds(pl.multiple_of(place * width, width), width)
        high_ref[rows, :] = high
        low_ref[rows, :] = low
        return carry

    lax.fori_loop(0, blocks, step, 0)


def prepare(matrix):
    rows, columns = matrix.shape
    width = 256
    half = pltpu.VMEM((columns, rows), jnp.bfloat16)
    return pl.pallas_call(
        prepare_kernel,
        out_shape=(half, half),
        in_specs=[pl.BlockSpec(memory_space=pltpu.HBM)],
        out_specs=(pl.BlockSpec(memory_space=pltpu.VMEM),) * 2,
        scratch_shapes=[
            pltpu.VMEM((columns // width, rows, width), jnp.float32),
            pltpu.SemaphoreType.DMA((columns // width,)),
        ],
        cost_estimate=pl.CostEstimate(flops=4_000_000_000, bytes_accessed=8 << 20, transcendentals=0),
        compiler_params=pltpu.CompilerParams(vmem_limit_bytes=24 << 20),
    )(pltpu.with_memory_space_constraint(matrix, pltpu.HBM))


def half_product(x_ref, high_ref, low_ref, which):
    x_high, x_low = split(x_ref[...])
    both = jnp.concatenate([x_high, x_low], axis=0)
    vectors, depth = x_high.shape
    rows = slice(which * depth, (which + 1) * depth)
    for start in range(0, high_ref.shape[1], 256):
        columns = slice(start, start + 256)
        first = jnp.dot(both, high_ref[rows, columns], preferred_element_type=jnp.float32)
        second = jnp.dot(x_high, low_ref[rows, columns], preferred_element_type=jnp.float32)
        yield columns, first[:vectors] + (first[vectors:] + second)


def first_kernel(x_ref, high_ref, low_ref, out_ref):
    for columns, total in half_product(x_ref, high_ref, low_ref, 0):
        out_ref[:, columns] = total


def second_kernel(x_ref, high_ref, low_ref, before_ref, out_ref):
    for columns, total in half_product(x_ref, high_ref, low_ref, 1):
        total = before_ref[:, columns] + total
        for copy in range(out_ref.shape[0]):
            out_ref[copy, :, columns] = total


def combine_kernel(scale, parts_ref, running_ref, summand_ref, total_ref):
    summand = parts_ref[0]
    for part in range(1, parts_ref.shape[0]):
        summand = summand + parts_ref[part]
    summand = summand / scale
    summand_ref[...] = summand
    total_ref[...] = running_ref[...] + summand


def call(kernel, out, flops, limit, *operands):
    vmem = pl.BlockSpec(memory_space=pltpu.VMEM)
    shapes = jax.tree.map(lambda shape: jax.ShapeDtypeStruct(shape, jnp.float32), out, is_leaf=lambda o: isinstance(o[0], int))
    return pl.pallas_call(
        kernel,
        out_shape=shapes,
        in_specs=[vmem] * len(operands),
        out_specs=jax.tree.map(lambda _: vmem, shapes),
        cost_estimate=pl.CostEstimate(flops=flops, bytes_accessed=4 << 20, transcendentals=0),
        compiler_params=pltpu.CompilerParams(vmem_limit_bytes=limit),
    )(*operands)


def product(block, halves):
    shape = block.shape
    other = lax.ppermute(block, ROW + COL, neighbour_moves())
    before = call(first_kernel, shape, 200_000_000, 4 << 20, block, *halves)
    return call(second_kernel, (8, *shape), 200_000_000, 4 << 20, other, *halves, before)


def local(matrix, vectors):
    shape = vectors.shape
    block = lax.ppermute(vectors, ROW + COL, owner_moves())
    halves = prepare(matrix)
    block, halves = lax.optimization_barrier((block, halves))
    running = vectors
    for degree in range(1, TERMS + 1):
        parts = lax.all_to_all(product(block, halves), COL, 0, 0, tiled=True)
        kernel = functools.partial(combine_kernel, float(degree * STEPS))
        summand, running = call(kernel, (shape, shape), 1_000_000, 2 << 20, parts, running)
        if degree < TERMS:
            block = lax.ppermute(summand, ROW + COL, owner_moves())
    return running


def solution(mesh):
    fine = Mesh(mesh.devices.reshape(tuple(SIZES.values())), tuple(SIZES))
    placed = (P(ROW, COL), P("rep", ROW))
    return jax.shard_map(local, mesh=fine, in_specs=placed, out_specs=P("rep", ROW), check_vma=False)
```

```python
import functools

import jax
import jax.numpy as jnp
from jax import lax
from jax.experimental import pallas as pl
from jax.experimental.pallas import tpu as pltpu
from jax.sharding import Mesh, PartitionSpec as P

TERMS = 6
STEPS = 1

ROW = ("xh", "zh", "zl")
COL = ("xl", "y")
SIZES = {"xh": 2, "zh": 4, "zl": 2, "xl": 2, "y": 4, "rep": 2}
PLACES = [
    (xh, zh, zl, xl, y)
    for xh in range(2)
    for zh in range(4)
    for zl in range(2)
    for xl in range(2)
    for y in range(4)
]
FAR = 2


def index(xh, zh, zl, xl, y):
    return (((xh * 4 + zh) * 2 + zl) * 2 + xl) * 4 + y


def owner_moves():
    def across(zh, y):
        return y if (y - zh) % 2 else (y + FAR) % 4

    return [
        (index(xh, zh, zl, xl, y), index(xl, across(zh, y), zl ^ int(y == zh), xh, zh))
        for xh, zh, zl, xl, y in PLACES
    ]


def partner_moves(which):
    return [
        (index(xh, zh, zl, xl, y), index(xh ^ (which // 2), zh, zl ^ (which % 2), xl, y))
        for xh, zh, zl, xl, y in PLACES
    ]


def split(value):
    high = value.astype(jnp.bfloat16)
    low = (value - high.astype(jnp.float32)).astype(jnp.bfloat16)
    return high, low


def prepare_kernel(which, a_ref, high_ref, low_ref, held, sems):
    blocks = held.shape[0]
    width = held.shape[2]
    swapped = lax.rem(lax.axis_index("y") + FAR, 4) == lax.axis_index("zh")
    half = lax.axis_index("zl") ^ swapped.astype(jnp.int32) ^ (which % 2)
    side = lax.axis_index("xh") ^ (which // 2)
    quarter = half * 2 + side

    def copy(block):
        column = pl.multiple_of(quarter * (blocks * width) + block * width, width)
        return pltpu.make_async_copy(a_ref.at[:, pl.ds(column, width)], held.at[block], sems.at[block])

    for block in range(blocks):
        copy(block).start()
    for block in range(blocks):
        copy(block).wait()
        high, low = split(held[block].T)
        rows = pl.ds(block * width, width)
        high_ref[rows, :] = high
        low_ref[rows, :] = low


def prepare(matrix, which):
    rows, columns = matrix.shape
    width = 256
    half = pltpu.VMEM((columns // 4, rows), jnp.bfloat16)
    return pl.pallas_call(
        functools.partial(prepare_kernel, which),
        out_shape=(half, half),
        in_specs=[pl.BlockSpec(memory_space=pltpu.HBM)],
        out_specs=(pl.BlockSpec(memory_space=pltpu.VMEM),) * 2,
        scratch_shapes=[
            pltpu.VMEM((columns // 4 // width, rows, width), jnp.float32),
            pltpu.SemaphoreType.DMA((columns // 4 // width,)),
        ],
        cost_estimate=pl.CostEstimate(flops=1_000_000_000, bytes_accessed=4 << 20, transcendentals=0),
        compiler_params=pltpu.CompilerParams(vmem_limit_bytes=8 << 20),
    )(pltpu.with_memory_space_constraint(matrix, pltpu.HBM))


def quarter_product(x_ref, high_ref, low_ref):
    x_high, x_low = split(x_ref[...])
    both = jnp.concatenate([x_high, x_low], axis=0)
    vectors = x_high.shape[0]
    for start in range(0, high_ref.shape[1], 256):
        columns = slice(start, start + 256)
        first = jnp.dot(both, high_ref[:, columns], preferred_element_type=jnp.float32)
        second = jnp.dot(x_high, low_ref[:, columns], preferred_element_type=jnp.float32)
        yield start, first[:vectors] + (first[vectors:] + second)


def first_kernel(x_ref, high_ref, low_ref, out_ref):
    for start, total in quarter_product(x_ref, high_ref, low_ref):
        out_ref[:, start : start + 256] = total


def next_kernel(x_ref, high_ref, low_ref, before_ref, out_ref):
    for start, total in quarter_product(x_ref, high_ref, low_ref):
        out_ref[:, start : start + 256] = before_ref[:, start : start + 256] + total


def spread_kernel(x_ref, high_ref, low_ref, before_ref, out_ref):
    width = out_ref.shape[2]
    for start, total in quarter_product(x_ref, high_ref, low_ref):
        total = before_ref[:, start : start + 256] + total
        side, within = divmod(start, width)
        for copy in range(4):
            out_ref[side * 4 + copy, :, within : within + 256] = total


def last_kernel(scale, x_ref, high_ref, low_ref, before_ref, running_ref, out_ref):
    width = running_ref.shape[1]
    mine = lax.axis_index("xl")
    first = lax.axis_index("y") == 0
    for start, total in quarter_product(x_ref, high_ref, low_ref):
        total = before_ref[:, start : start + 256] + total
        side, within = divmod(start, width)
        running = running_ref[:, within : within + 256]
        adds = jnp.logical_and(first, mine == side)
        total = total / scale + jnp.where(adds, running, jnp.zeros_like(running))
        for copy in range(8):
            out_ref[copy, :, start : start + 256] = total


def combine_kernel(scale, parts_ref, running_ref, summand_ref, total_ref):
    summand = parts_ref[0]
    for part in range(1, parts_ref.shape[0]):
        summand = summand + parts_ref[part]
    summand = summand / scale
    summand_ref[...] = summand
    total_ref[...] = running_ref[...] + summand


def call(kernel, out, flops, limit, *operands):
    vmem = pl.BlockSpec(memory_space=pltpu.VMEM)
    shapes = jax.tree.map(lambda shape: jax.ShapeDtypeStruct(shape, jnp.float32), out, is_leaf=lambda o: isinstance(o[0], int))
    return pl.pallas_call(
        kernel,
        out_shape=shapes,
        in_specs=[vmem] * len(operands),
        out_specs=jax.tree.map(lambda _: vmem, shapes),
        cost_estimate=pl.CostEstimate(flops=flops, bytes_accessed=4 << 20, transcendentals=0),
        compiler_params=pltpu.CompilerParams(vmem_limit_bytes=limit),
    )(*operands)


def product(piece, quarters, scale=None, running=None):
    vectors, width = piece.shape
    rows = quarters[0][0].shape[1]
    flops, limit = 100_000_000, 4 << 20
    others = [lax.ppermute(piece, ROW + COL, partner_moves(which)) for which in (1, 2, 3)]
    total = call(first_kernel, (vectors, rows), flops, limit, piece, *quarters[0])
    for which in (1, 2):
        total = call(next_kernel, (vectors, rows), flops, limit, others[which - 1], *quarters[which], total)
    if running is None:
        return call(spread_kernel, (8, vectors, width), flops, limit, others[2], *quarters[3], total)
    kernel = functools.partial(last_kernel, scale)
    return call(kernel, (8, vectors, rows), flops, limit, others[2], *quarters[3], total, running)


def move(piece):
    return lax.ppermute(piece, ROW + COL, owner_moves())


def exchange(value):
    return lax.all_to_all(value, COL, 0, 0, tiled=True)


def local(matrix, vectors):
    half = vectors.shape[1] // 2
    running = jnp.where(lax.axis_index("xl") == 0, vectors[:, :half], vectors[:, half:])
    piece = move(running)
    quarters = [prepare(matrix, which) for which in range(4)]
    for degree in range(1, TERMS):
        parts = exchange(product(piece, quarters))
        kernel = functools.partial(combine_kernel, float(degree * STEPS))
        summand, running = call(kernel, (running.shape,) * 2, 1_000_000, 2 << 20, parts, running)
        piece = move(summand)
    parts = exchange(product(piece, quarters, float(TERMS * STEPS), running))
    return functools.reduce(jnp.add, [parts[part] for part in range(8)])


def solution(mesh):
    fine = Mesh(mesh.devices.reshape(tuple(SIZES.values())), tuple(SIZES))
    placed = (P(ROW, COL), P("rep", ROW))
    return jax.shard_map(local, mesh=fine, in_specs=placed, out_specs=P("rep", ROW), check_vma=False)
```

```python
import functools

import jax
import jax.numpy as jnp
from jax import lax
from jax.experimental import pallas as pl
from jax.experimental.pallas import tpu as pltpu
from jax.sharding import Mesh, PartitionSpec as P

TERMS = 6
STEPS = 1

ROW = ("xh", "zh", "zl")
COL = ("xl", "y")
SIZES = {"xh": 2, "zh": 4, "zl": 2, "xl": 2, "y": 4, "rep": 2}
PLACES = [
    (xh, zh, zl, xl, y)
    for xh in range(2)
    for zh in range(4)
    for zl in range(2)
    for xl in range(2)
    for y in range(4)
]
FAR = 2


def index(xh, zh, zl, xl, y):
    return (((xh * 4 + zh) * 2 + zl) * 2 + xl) * 4 + y


def owner_moves():
    def across(zh, y):
        return y if (y - zh) % 2 else (y + FAR) % 4

    return [
        (index(xh, zh, zl, xl, y), index(xl, across(zh, y), zl ^ int(y == zh), xh, zh))
        for xh, zh, zl, xl, y in PLACES
    ]


def partner_moves(which):
    return [
        (index(xh, zh, zl, xl, y), index(xh ^ (which // 2), zh, zl ^ (which % 2), xl, y))
        for xh, zh, zl, xl, y in PLACES
    ]


def split(value):
    high = value.astype(jnp.bfloat16)
    low = (value - high.astype(jnp.float32)).astype(jnp.bfloat16)
    return high, low


def prepare_kernel(a_ref, high_ref, low_ref, held, sems):
    blocks = held.shape[0]
    width = held.shape[2]
    swapped = lax.rem(lax.axis_index("y") + FAR, 4) == lax.axis_index("zh")
    own_half = lax.axis_index("zl") ^ swapped.astype(jnp.int32)
    own_side = lax.axis_index("xh")

    def copy(block):
        column = pl.multiple_of(block * width, width)
        return pltpu.make_async_copy(a_ref.at[:, pl.ds(column, width)], held.at[block], sems.at[block])

    for block in range(blocks):
        copy(block).start()

    def step(block, carry):
        copy(block).wait()
        high, low = split(held[block].T)
        half, side, part = block // 4, lax.rem(block // 2, 2), lax.rem(block, 2)
        place = ((half ^ own_half) + 2 * (side ^ own_side)) * 2 + part
        rows = pl.ds(pl.multiple_of(place * width, width), width)
        high_ref[rows, :] = high
        low_ref[rows, :] = low
        return carry

    lax.fori_loop(0, blocks, step, 0)


def prepare(matrix):
    rows, columns = matrix.shape
    width = columns // 8
    half = pltpu.VMEM((columns, rows), jnp.bfloat16)
    return pl.pallas_call(
        prepare_kernel,
        out_shape=(half, half),
        in_specs=[pl.BlockSpec(memory_space=pltpu.HBM)],
        out_specs=(pl.BlockSpec(memory_space=pltpu.VMEM),) * 2,
        scratch_shapes=[
            pltpu.VMEM((8, rows, width), jnp.float32),
            pltpu.SemaphoreType.DMA((8,)),
        ],
        cost_estimate=pl.CostEstimate(flops=4_000_000_000, bytes_accessed=8 << 20, transcendentals=0),
        compiler_params=pltpu.CompilerParams(vmem_limit_bytes=24 << 20),
    )(pltpu.with_memory_space_constraint(matrix, pltpu.HBM))


def tiles(pieces, high_ref, low_ref, before_ref=None):
    depth = high_ref.shape[0] // 4
    operands = []
    for quarter, piece in pieces:
        x_high, x_low = split(piece)
        rows = slice(quarter * depth, (quarter + 1) * depth)
        operands.append((rows, x_high, jnp.concatenate([x_high, x_low], axis=0)))
    for start in range(0, high_ref.shape[1], 256):
        columns = slice(start, start + 256)
        total = None
        for rows, x_high, both in operands:
            vectors = x_high.shape[0]
            first = jnp.dot(both, high_ref[rows, columns], preferred_element_type=jnp.float32)
            second = jnp.dot(x_high, low_ref[rows, columns], preferred_element_type=jnp.float32)
            value = first[:vectors] + (first[vectors:] + second)
            total = value if total is None else total + value
        if before_ref is not None:
            total = before_ref[:, columns] + total
        yield start, total


def block_pieces(quarters, x_ref):
    width = x_ref.shape[1] // 2
    side = lax.axis_index("xh")
    at = [pl.multiple_of(place * width, width) for place in (side, 1 - side)]
    return [(quarter, x_ref[:, pl.ds(place, width)]) for quarter, place in zip(quarters, at)]


def store(start, total, out_ref):
    out_ref[:, start : start + 256] = total


def spread(start, total, out_ref):
    side, within = divmod(start, out_ref.shape[2])
    for copy in range(4):
        out_ref[side * 4 + copy, :, within : within + 256] = total


def own_block_kernel(x_ref, high_ref, low_ref, vectors_ref, out_ref, running_ref):
    width = running_ref.shape[1]
    running_ref[...] = vectors_ref[:, pl.ds(pl.multiple_of(lax.axis_index("xl") * width, width), width)]
    for start, total in tiles(block_pieces((0, 2), x_ref), high_ref, low_ref):
        store(start, total, out_ref)


def other_block_kernel(x_ref, high_ref, low_ref, before_ref, out_ref):
    for start, total in tiles(block_pieces((1, 3), x_ref), high_ref, low_ref, before_ref):
        spread(start, total, out_ref)


def own_kernel(x_ref, high_ref, low_ref, out_ref):
    for start, total in tiles([(0, x_ref[...])], high_ref, low_ref):
        store(start, total, out_ref)


def next_kernel(which, x_ref, high_ref, low_ref, before_ref, out_ref):
    for start, total in tiles([(which, x_ref[...])], high_ref, low_ref, before_ref):
        store(start, total, out_ref)


def spread_kernel(x_ref, high_ref, low_ref, before_ref, out_ref):
    for start, total in tiles([(3, x_ref[...])], high_ref, low_ref, before_ref):
        spread(start, total, out_ref)


def last_kernel(scale, x_ref, high_ref, low_ref, before_ref, running_ref, out_ref):
    width = running_ref.shape[1]
    mine = lax.axis_index("xl")
    first = lax.axis_index("y") == 0
    for start, total in tiles([(3, x_ref[...])], high_ref, low_ref, before_ref):
        side, within = divmod(start, width)
        running = running_ref[:, within : within + 256]
        adds = jnp.logical_and(first, mine == side)
        total = total / scale + jnp.where(adds, running, jnp.zeros_like(running))
        for copy in range(8):
            out_ref[copy, :, start : start + 256] = total


def combine_kernel(scale, parts_ref, running_ref, summand_ref, total_ref):
    summand = parts_ref[0]
    for part in range(1, parts_ref.shape[0]):
        summand = summand + parts_ref[part]
    summand = summand / scale
    summand_ref[...] = summand
    total_ref[...] = running_ref[...] + summand


def call(kernel, out, flops, limit, *operands):
    vmem = pl.BlockSpec(memory_space=pltpu.VMEM)
    shapes = jax.tree.map(lambda shape: jax.ShapeDtypeStruct(shape, jnp.float32), out, is_leaf=lambda o: isinstance(o[0], int))
    return pl.pallas_call(
        kernel,
        out_shape=shapes,
        in_specs=[vmem] * len(operands),
        out_specs=jax.tree.map(lambda _: vmem, shapes),
        cost_estimate=pl.CostEstimate(flops=flops, bytes_accessed=4 << 20, transcendentals=0),
        compiler_params=pltpu.CompilerParams(vmem_limit_bytes=limit),
    )(*operands)


def permute(value, moves):
    return lax.ppermute(value, ROW + COL, moves)


def exchange(value):
    return lax.all_to_all(value, COL, 0, 0, tiled=True)


FLOPS, LIMIT = 100_000_000, 4 << 20


def block_product(block, halves, vectors):
    count, width = block.shape
    other = permute(block, partner_moves(1))
    out = ((count, width), (count, width // 2))
    total, running = call(own_block_kernel, out, 2 * FLOPS, LIMIT, block, *halves, vectors)
    return call(other_block_kernel, (8, count, width // 2), 2 * FLOPS, LIMIT, other, *halves, total), running


def product(piece, halves, scale=None, running=None):
    vectors, width = piece.shape
    rows = halves[0].shape[1]
    others = [permute(piece, partner_moves(which)) for which in (1, 2, 3)]
    total = call(own_kernel, (vectors, rows), FLOPS, LIMIT, piece, *halves)
    for which in (1, 2):
        kernel = functools.partial(next_kernel, which)
        total = call(kernel, (vectors, rows), FLOPS, LIMIT, others[which - 1], *halves, total)
    if running is None:
        return call(spread_kernel, (8, vectors, width), FLOPS, LIMIT, others[2], *halves, total)
    kernel = functools.partial(last_kernel, scale)
    return call(kernel, (8, vectors, rows), FLOPS, LIMIT, others[2], *halves, total, running)


def local(matrix, vectors):
    block = permute(vectors, owner_moves())
    halves = prepare(matrix)
    block, halves = lax.optimization_barrier((block, halves))
    partial_value, running = block_product(block, halves, vectors)
    parts = exchange(partial_value)
    for degree in range(1, TERMS):
        kernel = functools.partial(combine_kernel, float(degree * STEPS))
        summand, running = call(kernel, (running.shape,) * 2, 1_000_000, 2 << 20, parts, running)
        piece = permute(summand, owner_moves())
        if degree + 1 < TERMS:
            parts = exchange(product(piece, halves))
    parts = exchange(product(piece, halves, float(TERMS * STEPS), running))
    return functools.reduce(jnp.add, [parts[part] for part in range(8)])


def solution(mesh):
    fine = Mesh(mesh.devices.reshape(tuple(SIZES.values())), tuple(SIZES))
    placed = (P(ROW, COL), P("rep", ROW))
    return jax.shard_map(local, mesh=fine, in_specs=placed, out_specs=P("rep", ROW), check_vma=False)
```

```python
import functools

import jax
import jax.numpy as jnp
from jax import lax
from jax.experimental import pallas as pl
from jax.experimental.pallas import tpu as pltpu
from jax.sharding import Mesh, PartitionSpec as P

TERMS = 6
STEPS = 1

ROW = ("xh", "zh", "zl")
COL = ("xl", "y")
SIZES = {"xh": 2, "zh": 4, "zl": 2, "xl": 2, "y": 4, "rep": 2}
PLACES = [
    (xh, zh, zl, xl, y)
    for xh in range(2)
    for zh in range(4)
    for zl in range(2)
    for xl in range(2)
    for y in range(4)
]
FAR = 2
HANDED = 8


def index(xh, zh, zl, xl, y):
    return (((xh * 4 + zh) * 2 + zl) * 2 + xl) * 4 + y


def owner_moves():
    def across(zh, y):
        return y if (y - zh) % 2 else (y + FAR) % 4

    return [
        (index(xh, zh, zl, xl, y), index(xl, across(zh, y), zl ^ int(y == zh), xh, zh))
        for xh, zh, zl, xl, y in PLACES
    ]


def partner_moves(which):
    return [
        (index(xh, zh, zl, xl, y), index(xh ^ (which // 2), zh, zl ^ (which % 2), xl, y))
        for xh, zh, zl, xl, y in PLACES
    ]


def split(value):
    high = value.astype(jnp.bfloat16)
    low = (value - high.astype(jnp.float32)).astype(jnp.bfloat16)
    return high, low


def prepare_kernel(a_ref, high_ref, low_ref, held, sems):
    blocks = held.shape[0]
    width = held.shape[2]
    swapped = lax.rem(lax.axis_index("y") + FAR, 4) == lax.axis_index("zh")
    own_half = lax.axis_index("zl") ^ swapped.astype(jnp.int32)
    own_side = lax.axis_index("xh")

    def copy(block):
        column = pl.multiple_of(block * width, width)
        return pltpu.make_async_copy(a_ref.at[:, pl.ds(column, width)], held.at[block], sems.at[block])

    for block in range(blocks):
        copy(block).start()

    def step(block, carry):
        copy(block).wait()
        high, low = split(held[block].T)
        half, side, part = block // 4, lax.rem(block // 2, 2), lax.rem(block, 2)
        place = ((half ^ own_half) + 2 * (side ^ own_side)) * 2 + part
        rows = pl.ds(pl.multiple_of(place * width, width), width)
        high_ref[rows, :] = high
        low_ref[rows, :] = low
        return carry

    lax.fori_loop(0, blocks, step, 0)


def prepare(matrix):
    rows, columns = matrix.shape
    width = columns // 8
    half = pltpu.VMEM((columns, rows), jnp.bfloat16)
    return pl.pallas_call(
        prepare_kernel,
        out_shape=(half, half),
        in_specs=[pl.BlockSpec(memory_space=pltpu.HBM)],
        out_specs=(pl.BlockSpec(memory_space=pltpu.VMEM),) * 2,
        scratch_shapes=[
            pltpu.VMEM((8, rows, width), jnp.float32),
            pltpu.SemaphoreType.DMA((8,)),
        ],
        cost_estimate=pl.CostEstimate(flops=4_000_000_000, bytes_accessed=8 << 20, transcendentals=0),
        compiler_params=pltpu.CompilerParams(vmem_limit_bytes=24 << 20),
    )(pltpu.with_memory_space_constraint(matrix, pltpu.HBM))


def tiles(pieces, high_ref, low_ref, before_ref=None):
    depth = high_ref.shape[0] // 4
    operands = []
    for quarter, piece in pieces:
        x_high = piece.astype(jnp.bfloat16)
        high = x_high.astype(jnp.float32)
        both = jnp.concatenate([high, piece - high], axis=0).astype(jnp.bfloat16)
        operands.append((slice(quarter * depth, (quarter + 1) * depth), x_high, both))

    def tile(columns):
        total = None
        for rows, x_high, both in operands:
            vectors = x_high.shape[0]
            first = jnp.dot(both, high_ref[rows, columns], preferred_element_type=jnp.float32)
            second = jnp.dot(x_high, low_ref[rows, columns], preferred_element_type=jnp.float32)
            value = first[:vectors] + (first[vectors:] + second)
            total = value if total is None else total + value
        return total if before_ref is None else before_ref[:, columns] + total

    return tile


def store(tile, out_ref):
    def step(number, carry):
        columns = pl.ds(pl.multiple_of(number * 256, 256), 256)
        out_ref[:, columns] = tile(columns)
        return carry

    lax.fori_loop(0, out_ref.shape[1] // 256, step, 0)


def spread(tile, out_ref):
    width = out_ref.shape[2]

    def step(side, carry):
        for within in range(0, width, 256):
            total = tile(pl.ds(pl.multiple_of(side * width + within, 256), 256))
            for copy in range(4):
                out_ref[side * 4 + copy, :, within : within + 256] = total
        return carry

    lax.fori_loop(0, 2, step, 0)


def block_pieces(quarters, x_ref):
    width = x_ref.shape[1] // 2
    side = lax.axis_index("xh")
    at = [pl.multiple_of(place * width, width) for place in (side, 1 - side)]
    return [(quarter, x_ref[:, pl.ds(place, width)]) for quarter, place in zip(quarters, at)]


def own_block_kernel(x_ref, high_ref, low_ref, vectors_ref, out_ref, running_ref):
    width = running_ref.shape[1]
    running_ref[...] = vectors_ref[:, pl.ds(pl.multiple_of(lax.axis_index("xl") * width, width), width)]
    store(tiles(block_pieces((0, 2), x_ref), high_ref, low_ref), out_ref)


def other_block_kernel(x_ref, high_ref, low_ref, before_ref, out_ref):
    spread(tiles(block_pieces((1, 3), x_ref), high_ref, low_ref, before_ref), out_ref)


def own_kernel(x_ref, high_ref, low_ref, out_ref):
    store(tiles([(0, x_ref[...])], high_ref, low_ref), out_ref)


def next_kernel(which, x_ref, high_ref, low_ref, before_ref, out_ref):
    store(tiles([(which, x_ref[...])], high_ref, low_ref, before_ref), out_ref)


def spread_kernel(x_ref, high_ref, low_ref, before_ref, out_ref):
    spread(tiles([(3, x_ref[...])], high_ref, low_ref, before_ref), out_ref)


def last_kernel(scale, x_ref, high_ref, low_ref, before_ref, running_ref, out_ref):
    width = running_ref.shape[1]
    mine = lax.axis_index("xl")
    first = lax.axis_index("y") == 0
    tile = tiles([(3, x_ref[...])], high_ref, low_ref, before_ref)

    def step(side, carry):
        for within in range(0, width, 256):
            columns = pl.ds(pl.multiple_of(side * width + within, 256), 256)
            running = running_ref[:, within : within + 256]
            adds = jnp.logical_and(first, mine == side)
            total = tile(columns) / scale + jnp.where(adds, running, jnp.zeros_like(running))
            for copy in range(8):
                out_ref[copy, :, columns] = total
        return carry

    lax.fori_loop(0, 2, step, 0)


def combine_kernel(scale, parts_ref, running_ref, summand_ref, total_ref):
    summand = parts_ref[0]
    for part in range(1, parts_ref.shape[0]):
        summand = summand + parts_ref[part]
    summand = summand / scale
    summand_ref[...] = summand
    total_ref[...] = running_ref[...] + summand


def call(kernel, out, flops, limit, *operands):
    vmem = pl.BlockSpec(memory_space=pltpu.VMEM)
    shapes = jax.tree.map(lambda shape: jax.ShapeDtypeStruct(shape, jnp.float32), out, is_leaf=lambda o: isinstance(o[0], int))
    return pl.pallas_call(
        kernel,
        out_shape=shapes,
        in_specs=[vmem] * len(operands),
        out_specs=jax.tree.map(lambda _: vmem, shapes),
        cost_estimate=pl.CostEstimate(flops=flops, bytes_accessed=4 << 20, transcendentals=0),
        compiler_params=pltpu.CompilerParams(vmem_limit_bytes=limit),
    )(*operands)


def permute(value, moves, rep):
    pairs = [(source * 2 + rep, target * 2 + rep) for source, target in moves]
    return lax.ppermute(value, ROW + COL + ("rep",), pairs)


def exchange(value):
    return lax.all_to_all(value, COL, 0, 0, tiled=True)


FLOPS, LIMIT = 100_000_000, 4 << 20


def block_product(block, halves, vectors, rep):
    count, width = block.shape
    other = permute(block, partner_moves(1), rep)
    out = ((count, width), (count, width // 2))
    total, running = call(own_block_kernel, out, 2 * FLOPS, LIMIT, block, *halves, vectors)
    return call(other_block_kernel, (8, count, width // 2), 2 * FLOPS, LIMIT, other, *halves, total), running


def product(piece, halves, rep, scale=None, running=None):
    vectors, width = piece.shape
    rows = halves[0].shape[1]
    others = [permute(piece, partner_moves(which), rep) for which in (1, 2, 3)]
    total = call(own_kernel, (vectors, rows), FLOPS, LIMIT, piece, *halves)
    for which in (1, 2):
        kernel = functools.partial(next_kernel, which)
        total = call(kernel, (vectors, rows), FLOPS, LIMIT, others[which - 1], *halves, total)
    if running is None:
        return call(spread_kernel, (8, vectors, width), FLOPS, LIMIT, others[2], *halves, total)
    kernel = functools.partial(last_kernel, scale)
    return call(kernel, (8, vectors, rows), FLOPS, LIMIT, others[2], *halves, total, running)


def series(matrix, vectors, rep):
    block = permute(vectors, owner_moves(), rep)
    halves = prepare(matrix)
    block, halves = lax.optimization_barrier((block, halves))
    partial_value, running = block_product(block, halves, vectors, rep)
    parts = exchange(partial_value)
    for degree in range(1, TERMS):
        kernel = functools.partial(combine_kernel, float(degree * STEPS))
        summand, running = call(kernel, (running.shape,) * 2, 1_000_000, 2 << 20, parts, running)
        piece = permute(summand, owner_moves(), rep)
        if degree + 1 < TERMS:
            parts = exchange(product(piece, halves, rep))
    parts = exchange(product(piece, halves, rep, float(TERMS * STEPS), running))
    return functools.reduce(jnp.add, [parts[part] for part in range(8)])


def local(matrix, vectors):
    count = vectors.shape[0]
    kept = count - HANDED
    handed = lax.ppermute(vectors[kept:], "rep", [(0, 1)])

    def most(matrix, vectors, handed):
        result = series(matrix, jnp.concatenate([vectors, handed], axis=0), 1)
        return result[:count], result[count:]

    def fewer(matrix, vectors, handed):
        result, handed = lax.optimization_barrier((series(matrix, vectors[:kept], 0), handed))
        return jnp.concatenate([result, handed], axis=0), handed

    takes = lax.axis_index("rep") == 1
    result, handed = lax.cond(takes, most, fewer, matrix, vectors, handed)
    back = lax.ppermute(handed, "rep", [(1, 0)])
    return jnp.concatenate([result[:kept], jnp.where(takes, result[kept:], back)], axis=0)


def solution(mesh):
    fine = Mesh(mesh.devices.reshape(tuple(SIZES.values())), tuple(SIZES))
    placed = (P(ROW, COL), P("rep", ROW))
    return jax.shard_map(local, mesh=fine, in_specs=placed, out_specs=P("rep", ROW), check_vma=False)
```

```python
import functools

import jax
import jax.numpy as jnp
from jax import lax
from jax.experimental import pallas as pl
from jax.experimental.pallas import tpu as pltpu
from jax.sharding import Mesh, PartitionSpec as P

TERMS = 6
STEPS = 1

ROW = ("xh", "zh", "zl")
COL = ("xl", "y")
SIZES = {"xh": 2, "zh": 4, "zl": 2, "xl": 2, "y": 4, "rep": 2}
PLACES = [
    (xh, zh, zl, xl, y)
    for xh in range(2)
    for zh in range(4)
    for zl in range(2)
    for xl in range(2)
    for y in range(4)
]
FAR = 2
HANDED = 8


def index(xh, zh, zl, xl, y):
    return (((xh * 4 + zh) * 2 + zl) * 2 + xl) * 4 + y


def owner_moves():
    def across(zh, y):
        return y if (y - zh) % 2 else (y + FAR) % 4

    return [
        (index(xh, zh, zl, xl, y), index(xl, across(zh, y), zl ^ int(y == zh), xh, zh))
        for xh, zh, zl, xl, y in PLACES
    ]


def partner_moves(which):
    return [
        (index(xh, zh, zl, xl, y), index(xh ^ (which // 2), zh, zl ^ (which % 2), xl, y))
        for xh, zh, zl, xl, y in PLACES
    ]


def split(value):
    high = value.astype(jnp.bfloat16)
    low = (value - high.astype(jnp.float32)).astype(jnp.bfloat16)
    return high, low


def prepare_kernel(a_ref, high_ref, low_ref, held, sems):
    blocks = held.shape[0]
    width = held.shape[2]
    swapped = lax.rem(lax.axis_index("y") + FAR, 4) == lax.axis_index("zh")
    own_half = lax.axis_index("zl") ^ swapped.astype(jnp.int32)
    own_side = lax.axis_index("xh")

    def copy(block):
        column = pl.multiple_of(block * width, width)
        return pltpu.make_async_copy(a_ref.at[:, pl.ds(column, width)], held.at[block], sems.at[block])

    for block in range(blocks):
        copy(block).start()

    def step(block, carry):
        copy(block).wait()
        high, low = split(held[block].T)
        half, side, part = block // 4, lax.rem(block // 2, 2), lax.rem(block, 2)
        place = ((half ^ own_half) + 2 * (side ^ own_side)) * 2 + part
        rows = pl.ds(pl.multiple_of(place * width, width), width)
        high_ref[rows, :] = high
        low_ref[rows, :] = low
        return carry

    lax.fori_loop(0, blocks, step, 0)


def prepare(matrix):
    rows, columns = matrix.shape
    width = columns // 8
    half = pltpu.VMEM((columns, rows), jnp.bfloat16)
    return pl.pallas_call(
        prepare_kernel,
        out_shape=(half, half),
        in_specs=[pl.BlockSpec(memory_space=pltpu.HBM)],
        out_specs=(pl.BlockSpec(memory_space=pltpu.VMEM),) * 2,
        scratch_shapes=[
            pltpu.VMEM((8, rows, width), jnp.float32),
            pltpu.SemaphoreType.DMA((8,)),
        ],
        cost_estimate=pl.CostEstimate(flops=4_000_000_000, bytes_accessed=8 << 20, transcendentals=0),
        compiler_params=pltpu.CompilerParams(vmem_limit_bytes=24 << 20),
    )(pltpu.with_memory_space_constraint(matrix, pltpu.HBM))


def tiles(pieces, high_ref, low_ref, before_ref=None):
    depth = high_ref.shape[0] // 4
    operands = []
    for quarter, piece in pieces:
        x_high = piece.astype(jnp.bfloat16)
        high = x_high.astype(jnp.float32)
        both = jnp.concatenate([high, piece - high], axis=0).astype(jnp.bfloat16)
        operands.append((slice(quarter * depth, (quarter + 1) * depth), x_high, both))

    def tile(columns):
        total = None
        for rows, x_high, both in operands:
            vectors = x_high.shape[0]
            first = jnp.dot(both, high_ref[rows, columns], preferred_element_type=jnp.float32)
            second = jnp.dot(x_high, low_ref[rows, columns], preferred_element_type=jnp.float32)
            value = first[:vectors] + (first[vectors:] + second)
            total = value if total is None else total + value
        return total if before_ref is None else before_ref[:, columns] + total

    return tile


def store(tile, out_ref):
    def step(number, carry):
        columns = pl.ds(pl.multiple_of(number * 256, 256), 256)
        out_ref[:, columns] = tile(columns)
        return carry

    lax.fori_loop(0, out_ref.shape[1] // 256, step, 0)


def spread(tile, out_ref):
    width = out_ref.shape[2]

    def step(side, carry):
        for within in range(0, width, 256):
            total = tile(pl.ds(pl.multiple_of(side * width + within, 256), 256))
            for copy in range(4):
                out_ref[side * 4 + copy, :, within : within + 256] = total
        return carry

    lax.fori_loop(0, 2, step, 0)


def block_pieces(quarters, x_ref):
    width = x_ref.shape[1] // 2
    side = lax.axis_index("xh")
    at = [pl.multiple_of(place * width, width) for place in (side, 1 - side)]
    return [(quarter, x_ref[:, pl.ds(place, width)]) for quarter, place in zip(quarters, at)]


def own_block_kernel(x_ref, high_ref, low_ref, vectors_ref, out_ref, running_ref):
    width = running_ref.shape[1]
    running_ref[...] = vectors_ref[:, pl.ds(pl.multiple_of(lax.axis_index("xl") * width, width), width)]
    store(tiles(block_pieces((0, 2), x_ref), high_ref, low_ref), out_ref)


def other_block_kernel(x_ref, high_ref, low_ref, before_ref, out_ref):
    spread(tiles(block_pieces((1, 3), x_ref), high_ref, low_ref, before_ref), out_ref)


def own_kernel(x_ref, high_ref, low_ref, out_ref):
    store(tiles([(0, x_ref[...])], high_ref, low_ref), out_ref)


def next_kernel(which, x_ref, high_ref, low_ref, before_ref, out_ref):
    store(tiles([(which, x_ref[...])], high_ref, low_ref, before_ref), out_ref)


def spread_kernel(x_ref, high_ref, low_ref, before_ref, out_ref):
    spread(tiles([(3, x_ref[...])], high_ref, low_ref, before_ref), out_ref)


def last_kernel(scale, x_ref, high_ref, low_ref, before_ref, running_ref, out_ref):
    width = running_ref.shape[1]
    mine = lax.axis_index("xl")
    first = lax.axis_index("y") == 0
    tile = tiles([(3, x_ref[...])], high_ref, low_ref, before_ref)

    def step(side, carry):
        for within in range(0, width, 256):
            columns = pl.ds(pl.multiple_of(side * width + within, 256), 256)
            running = running_ref[:, within : within + 256]
            adds = jnp.logical_and(first, mine == side)
            total = tile(columns) / scale + jnp.where(adds, running, jnp.zeros_like(running))
            for copy in range(8):
                out_ref[copy, :, columns] = total
        return carry

    lax.fori_loop(0, 2, step, 0)


def combine_kernel(scale, parts_ref, running_ref, summand_ref, total_ref):
    summand = parts_ref[0]
    for part in range(1, parts_ref.shape[0]):
        summand = summand + parts_ref[part]
    summand = summand / scale
    summand_ref[...] = summand
    total_ref[...] = running_ref[...] + summand


def call(kernel, out, flops, limit, *operands):
    vmem = pl.BlockSpec(memory_space=pltpu.VMEM)
    shapes = jax.tree.map(lambda shape: jax.ShapeDtypeStruct(shape, jnp.float32), out, is_leaf=lambda o: isinstance(o[0], int))
    return pl.pallas_call(
        kernel,
        out_shape=shapes,
        in_specs=[vmem] * len(operands),
        out_specs=jax.tree.map(lambda _: vmem, shapes),
        cost_estimate=pl.CostEstimate(flops=flops, bytes_accessed=4 << 20, transcendentals=0),
        compiler_params=pltpu.CompilerParams(vmem_limit_bytes=limit),
    )(*operands)


def permute(value, moves):
    return lax.ppermute(value, ROW + COL, moves)


def exchange(value):
    return lax.all_to_all(value, COL, 0, 0, tiled=True)


FLOPS, LIMIT = 100_000_000, 4 << 20


def block_product(block, halves, vectors):
    count, width = block.shape
    other = permute(block, partner_moves(1))
    out = ((count, width), (count, width // 2))
    total, running = call(own_block_kernel, out, 2 * FLOPS, LIMIT, block, *halves, vectors)
    return call(other_block_kernel, (8, count, width // 2), 2 * FLOPS, LIMIT, other, *halves, total), running


def product(piece, halves, scale=None, running=None):
    vectors, width = piece.shape
    rows = halves[0].shape[1]
    others = [permute(piece, partner_moves(which)) for which in (1, 2, 3)]
    total = call(own_kernel, (vectors, rows), FLOPS, LIMIT, piece, *halves)
    for which in (1, 2):
        kernel = functools.partial(next_kernel, which)
        total = call(kernel, (vectors, rows), FLOPS, LIMIT, others[which - 1], *halves, total)
    if running is None:
        return call(spread_kernel, (8, vectors, width), FLOPS, LIMIT, others[2], *halves, total)
    kernel = functools.partial(last_kernel, scale)
    return call(kernel, (8, vectors, rows), FLOPS, LIMIT, others[2], *halves, total, running)


def series(matrix, vectors):
    block = permute(vectors, owner_moves())
    halves = prepare(matrix)
    block, halves = lax.optimization_barrier((block, halves))
    partial_value, running = block_product(block, halves, vectors)
    parts = exchange(partial_value)
    for degree in range(1, TERMS):
        kernel = functools.partial(combine_kernel, float(degree * STEPS))
        summand, running = call(kernel, (running.shape,) * 2, 1_000_000, 2 << 20, parts, running)
        piece = permute(summand, owner_moves())
        if degree + 1 < TERMS:
            parts = exchange(product(piece, halves))
    parts = exchange(product(piece, halves, float(TERMS * STEPS), running))
    return functools.reduce(jnp.add, [parts[part] for part in range(8)])


def local(matrix, vectors):
    count = vectors.shape[0]
    kept = count - HANDED
    handed = lax.ppermute(vectors[kept:], "rep", [(0, 1)])

    def most(matrix, vectors, handed):
        result = series(matrix, jnp.concatenate([vectors, handed], axis=0))
        return result[:count], result[count:]

    def fewer(matrix, vectors, handed):
        result, handed = lax.optimization_barrier((series(matrix, vectors[:kept]), handed))
        return jnp.concatenate([result, handed], axis=0), handed

    takes = lax.axis_index("rep") == 1
    result, handed = lax.cond(takes, most, fewer, matrix, vectors, handed)
    back = lax.ppermute(handed, "rep", [(1, 0)])
    return jnp.concatenate([result[:kept], jnp.where(takes, result[kept:], back)], axis=0)


def solution(mesh):
    fine = Mesh(mesh.devices.reshape(tuple(SIZES.values())), tuple(SIZES))
    placed = (P(ROW, COL), P("rep", ROW))
    return jax.shard_map(local, mesh=fine, in_specs=placed, out_specs=P("rep", ROW), check_vma=False)
```

```python
import functools

import jax
import jax.numpy as jnp
from jax import lax
from jax.experimental import pallas as pl
from jax.experimental.pallas import tpu as pltpu
from jax.sharding import Mesh, PartitionSpec as P

TERMS = 6
STEPS = 1

ROW = ("xh", "zh", "zl")
COL = ("xl", "y")
SIZES = {"xh": 2, "zh": 4, "zl": 2, "xl": 2, "y": 4, "rep": 2}
PLACES = [
    (xh, zh, zl, xl, y)
    for xh in range(2)
    for zh in range(4)
    for zl in range(2)
    for xl in range(2)
    for y in range(4)
]
FAR = 2
ARRIVALS = (1, 3, 2)


def index(xh, zh, zl, xl, y):
    return (((xh * 4 + zh) * 2 + zl) * 2 + xl) * 4 + y


def owner_moves():
    def across(zh, y):
        return y if (y - zh) % 2 else (y + FAR) % 4

    return [
        (index(xh, zh, zl, xl, y), index(xl, across(zh, y), zl ^ int(y == zh), xh, zh))
        for xh, zh, zl, xl, y in PLACES
    ]


def partner_moves(which):
    return [
        (index(xh, zh, zl, xl, y), index(xh ^ (which // 2), zh, zl ^ (which % 2), xl, y))
        for xh, zh, zl, xl, y in PLACES
    ]


def split(value):
    high = value.astype(jnp.bfloat16)
    low = (value - high.astype(jnp.float32)).astype(jnp.bfloat16)
    return high, low


def prepare_kernel(a_ref, high_ref, low_ref, held, sems):
    blocks = held.shape[0]
    width = held.shape[2]
    swapped = lax.rem(lax.axis_index("y") + FAR, 4) == lax.axis_index("zh")
    own_half = lax.axis_index("zl") ^ swapped.astype(jnp.int32)
    own_side = lax.axis_index("xh")

    def copy(block):
        column = pl.multiple_of(block * width, width)
        return pltpu.make_async_copy(a_ref.at[:, pl.ds(column, width)], held.at[block], sems.at[block])

    for block in range(blocks):
        copy(block).start()

    def step(block, carry):
        copy(block).wait()
        high, low = split(held[block].T)
        half, side, part = block // 4, lax.rem(block // 2, 2), lax.rem(block, 2)
        place = ((half ^ own_half) + 2 * (side ^ own_side)) * 2 + part
        rows = pl.ds(pl.multiple_of(place * width, width), width)
        high_ref[rows, :] = high
        low_ref[rows, :] = low
        return carry

    lax.fori_loop(0, blocks, step, 0)


def prepare(matrix):
    rows, columns = matrix.shape
    width = columns // 8
    half = pltpu.VMEM((columns, rows), jnp.bfloat16)
    return pl.pallas_call(
        prepare_kernel,
        out_shape=(half, half),
        in_specs=[pl.BlockSpec(memory_space=pltpu.HBM)],
        out_specs=(pl.BlockSpec(memory_space=pltpu.VMEM),) * 2,
        scratch_shapes=[
            pltpu.VMEM((8, rows, width), jnp.float32),
            pltpu.SemaphoreType.DMA((8,)),
        ],
        cost_estimate=pl.CostEstimate(flops=4_000_000_000, bytes_accessed=8 << 20, transcendentals=0),
        compiler_params=pltpu.CompilerParams(vmem_limit_bytes=24 << 20),
    )(pltpu.with_memory_space_constraint(matrix, pltpu.HBM))


def tiles(pieces, high_ref, low_ref, before_ref=None):
    depth = high_ref.shape[0] // 4
    operands = []
    for quarter, piece in pieces:
        x_high, x_low = split(piece)
        rows = slice(quarter * depth, (quarter + 1) * depth)
        operands.append((rows, x_high, jnp.concatenate([x_high, x_low], axis=0)))
    for start in range(0, high_ref.shape[1], 256):
        columns = slice(start, start + 256)
        total = None
        for rows, x_high, both in operands:
            vectors = x_high.shape[0]
            first = jnp.dot(both, high_ref[rows, columns], preferred_element_type=jnp.float32)
            second = jnp.dot(x_high, low_ref[rows, columns], preferred_element_type=jnp.float32)
            value = first[:vectors] + (first[vectors:] + second)
            total = value if total is None else total + value
        if before_ref is not None:
            total = before_ref[:, columns] + total
        yield start, total


def block_pieces(quarters, x_ref):
    width = x_ref.shape[1] // 2
    side = lax.axis_index("xh")
    at = [pl.multiple_of(place * width, width) for place in (side, 1 - side)]
    return [(quarter, x_ref[:, pl.ds(place, width)]) for quarter, place in zip(quarters, at)]


def store(start, total, out_ref):
    out_ref[:, start : start + 256] = total


def spread(start, total, out_ref):
    side, within = divmod(start, out_ref.shape[2])
    for copy in range(4):
        out_ref[copy * 2 + side, :, within : within + 256] = total


def own_block_kernel(x_ref, high_ref, low_ref, vectors_ref, out_ref, running_ref):
    width = running_ref.shape[1]
    running_ref[...] = vectors_ref[:, pl.ds(pl.multiple_of(lax.axis_index("xl") * width, width), width)]
    for start, total in tiles(block_pieces((0, 2), x_ref), high_ref, low_ref):
        store(start, total, out_ref)


def other_block_kernel(x_ref, high_ref, low_ref, before_ref, out_ref):
    for start, total in tiles(block_pieces((1, 3), x_ref), high_ref, low_ref, before_ref):
        spread(start, total, out_ref)


def own_kernel(x_ref, high_ref, low_ref, out_ref):
    for start, total in tiles([(0, x_ref[...])], high_ref, low_ref):
        store(start, total, out_ref)


def next_kernel(which, x_ref, high_ref, low_ref, before_ref, out_ref):
    for start, total in tiles([(which, x_ref[...])], high_ref, low_ref, before_ref):
        store(start, total, out_ref)


def spread_kernel(which, x_ref, high_ref, low_ref, before_ref, out_ref):
    for start, total in tiles([(which, x_ref[...])], high_ref, low_ref, before_ref):
        spread(start, total, out_ref)


def last_kernel(which, scale, x_ref, high_ref, low_ref, before_ref, running_ref, out_ref):
    width = running_ref.shape[1]
    mine = lax.axis_index("xl")
    first = lax.axis_index("y") == 0
    for start, total in tiles([(which, x_ref[...])], high_ref, low_ref, before_ref):
        side, within = divmod(start, width)
        running = running_ref[:, within : within + 256]
        adds = jnp.logical_and(first, mine == side)
        total = total / scale + jnp.where(adds, running, jnp.zeros_like(running))
        for copy in range(8):
            out_ref[copy, :, start : start + 256] = total


def combine_kernel(scale, parts_ref, running_ref, summand_ref, total_ref):
    summand = parts_ref[0]
    for part in range(1, parts_ref.shape[0]):
        summand = summand + parts_ref[part]
    summand = summand / scale
    summand_ref[...] = summand
    total_ref[...] = running_ref[...] + summand


def call(kernel, out, flops, limit, *operands):
    vmem = pl.BlockSpec(memory_space=pltpu.VMEM)
    shapes = jax.tree.map(lambda shape: jax.ShapeDtypeStruct(shape, jnp.float32), out, is_leaf=lambda o: isinstance(o[0], int))
    return pl.pallas_call(
        kernel,
        out_shape=shapes,
        in_specs=[vmem] * len(operands),
        out_specs=jax.tree.map(lambda _: vmem, shapes),
        cost_estimate=pl.CostEstimate(flops=flops, bytes_accessed=4 << 20, transcendentals=0),
        compiler_params=pltpu.CompilerParams(vmem_limit_bytes=limit),
    )(*operands)


def permute(value, moves):
    return lax.ppermute(value, ROW + COL, moves)


def exchange(value):
    return lax.all_to_all(value, ("y", "xl"), 0, 0, tiled=True)


FLOPS, LIMIT = 100_000_000, 4 << 20


def block_product(block, halves, vectors):
    count, width = block.shape
    other = permute(block, partner_moves(1))
    out = ((count, width), (count, width // 2))
    total, running = call(own_block_kernel, out, 2 * FLOPS, LIMIT, block, *halves, vectors)
    return call(other_block_kernel, (8, count, width // 2), 2 * FLOPS, LIMIT, other, *halves, total), running


def product(piece, halves, scale=None, running=None):
    vectors, width = piece.shape
    rows = halves[0].shape[1]
    others = {}
    for which in ARRIVALS:
        others[which] = permute(piece, partner_moves(which))
    total = call(own_kernel, (vectors, rows), FLOPS, LIMIT, piece, *halves)
    for which in ARRIVALS[:2]:
        kernel = functools.partial(next_kernel, which)
        total = call(kernel, (vectors, rows), FLOPS, LIMIT, others[which], *halves, total)
    which = ARRIVALS[2]
    if running is None:
        kernel = functools.partial(spread_kernel, which)
        return call(kernel, (8, vectors, width), FLOPS, LIMIT, others[which], *halves, total)
    kernel = functools.partial(last_kernel, which, scale)
    return call(kernel, (8, vectors, rows), FLOPS, LIMIT, others[which], *halves, total, running)


def local(matrix, vectors):
    block = permute(vectors, owner_moves())
    halves = prepare(matrix)
    block, halves = lax.optimization_barrier((block, halves))
    partial_value, running = block_product(block, halves, vectors)
    parts = exchange(partial_value)
    for degree in range(1, TERMS):
        kernel = functools.partial(combine_kernel, float(degree * STEPS))
        summand, running = call(kernel, (running.shape,) * 2, 1_000_000, 2 << 20, parts, running)
        piece = permute(summand, owner_moves())
        if degree + 1 < TERMS:
            parts = exchange(product(piece, halves))
        else:
            parts = exchange(product(piece, halves, float(TERMS * STEPS), running))
    return functools.reduce(jnp.add, [parts[part] for part in range(8)])


def solution(mesh):
    fine = Mesh(mesh.devices.reshape(tuple(SIZES.values())), tuple(SIZES))
    placed = (P(ROW, COL), P("rep", ROW))
    return jax.shard_map(local, mesh=fine, in_specs=placed, out_specs=P("rep", ROW), check_vma=False)
```

```python
import functools

import jax
import jax.numpy as jnp
from jax import lax
from jax.experimental import pallas as pl
from jax.experimental.pallas import tpu as pltpu
from jax.sharding import Mesh, PartitionSpec as P

TERMS = 6
STEPS = 1

ROW = ("xh", "zh", "zl")
COL = ("xl", "y")
SIZES = {"xh": 2, "zh": 4, "zl": 2, "xl": 2, "y": 4, "rep": 2}
PLACES = [
    (xh, zh, zl, xl, y)
    for xh in range(2)
    for zh in range(4)
    for zl in range(2)
    for xl in range(2)
    for y in range(4)
]
FAR = 2
ARRIVALS = (3, 2, 1)


def index(xh, zh, zl, xl, y):
    return (((xh * 4 + zh) * 2 + zl) * 2 + xl) * 4 + y


def owner_moves():
    def across(zh, y):
        return y if (y - zh) % 2 else (y + FAR) % 4

    return [
        (index(xh, zh, zl, xl, y), index(xl, across(zh, y), zl ^ int(y == zh), xh, zh))
        for xh, zh, zl, xl, y in PLACES
    ]


def partner_moves(which):
    return [
        (index(xh, zh, zl, xl, y), index(xh ^ (which // 2), zh, zl ^ (which % 2), xl, y))
        for xh, zh, zl, xl, y in PLACES
    ]


def split(value):
    high = value.astype(jnp.bfloat16)
    low = (value - high.astype(jnp.float32)).astype(jnp.bfloat16)
    return high, low


def prepare_kernel(a_ref, high_ref, low_ref, held, sems):
    blocks = held.shape[0]
    width = held.shape[2]
    swapped = lax.rem(lax.axis_index("y") + FAR, 4) == lax.axis_index("zh")
    own_half = lax.axis_index("zl") ^ swapped.astype(jnp.int32)
    own_side = lax.axis_index("xh")

    def copy(block):
        column = pl.multiple_of(block * width, width)
        return pltpu.make_async_copy(a_ref.at[:, pl.ds(column, width)], held.at[block], sems.at[block])

    for block in range(blocks):
        copy(block).start()

    def step(block, carry):
        copy(block).wait()
        high, low = split(held[block].T)
        half, side, part = block // 4, lax.rem(block // 2, 2), lax.rem(block, 2)
        place = ((half ^ own_half) + 2 * (side ^ own_side)) * 2 + part
        rows = pl.ds(pl.multiple_of(place * width, width), width)
        high_ref[rows, :] = high
        low_ref[rows, :] = low
        return carry

    lax.fori_loop(0, blocks, step, 0)


def prepare(matrix):
    rows, columns = matrix.shape
    width = columns // 8
    half = pltpu.VMEM((columns, rows), jnp.bfloat16)
    return pl.pallas_call(
        prepare_kernel,
        out_shape=(half, half),
        in_specs=[pl.BlockSpec(memory_space=pltpu.HBM)],
        out_specs=(pl.BlockSpec(memory_space=pltpu.VMEM),) * 2,
        scratch_shapes=[
            pltpu.VMEM((8, rows, width), jnp.float32),
            pltpu.SemaphoreType.DMA((8,)),
        ],
        cost_estimate=pl.CostEstimate(flops=4_000_000_000, bytes_accessed=8 << 20, transcendentals=0),
        compiler_params=pltpu.CompilerParams(vmem_limit_bytes=24 << 20),
    )(pltpu.with_memory_space_constraint(matrix, pltpu.HBM))


def tiles(pieces, high_ref, low_ref, before_ref=None):
    depth = high_ref.shape[0] // 4
    operands = []
    for quarter, piece in pieces:
        x_high, x_low = split(piece)
        rows = slice(quarter * depth, (quarter + 1) * depth)
        operands.append((rows, x_high, jnp.concatenate([x_high, x_low], axis=0)))
    for start in range(0, high_ref.shape[1], 256):
        columns = slice(start, start + 256)
        total = None
        for rows, x_high, both in operands:
            vectors = x_high.shape[0]
            first = jnp.dot(both, high_ref[rows, columns], preferred_element_type=jnp.float32)
            second = jnp.dot(x_high, low_ref[rows, columns], preferred_element_type=jnp.float32)
            value = first[:vectors] + (first[vectors:] + second)
            total = value if total is None else total + value
        if before_ref is not None:
            total = before_ref[:, columns] + total
        yield start, total


def block_pieces(quarters, x_ref):
    width = x_ref.shape[1] // 2
    side = lax.axis_index("xh")
    at = [pl.multiple_of(place * width, width) for place in (side, 1 - side)]
    return [(quarter, x_ref[:, pl.ds(place, width)]) for quarter, place in zip(quarters, at)]


def store(start, total, out_ref):
    out_ref[:, start : start + 256] = total


def spread(start, total, out_ref):
    side, within = divmod(start, out_ref.shape[2])
    for copy in range(4):
        out_ref[side * 4 + copy, :, within : within + 256] = total


def own_block_kernel(x_ref, high_ref, low_ref, vectors_ref, out_ref, running_ref):
    width = running_ref.shape[1]
    running_ref[...] = vectors_ref[:, pl.ds(pl.multiple_of(lax.axis_index("xl") * width, width), width)]
    for start, total in tiles(block_pieces((0, 2), x_ref), high_ref, low_ref):
        store(start, total, out_ref)


def other_block_kernel(x_ref, high_ref, low_ref, before_ref, out_ref):
    for start, total in tiles(block_pieces((1, 3), x_ref), high_ref, low_ref, before_ref):
        spread(start, total, out_ref)


def own_kernel(x_ref, high_ref, low_ref, out_ref):
    for start, total in tiles([(0, x_ref[...])], high_ref, low_ref):
        store(start, total, out_ref)


def next_kernel(which, x_ref, high_ref, low_ref, before_ref, out_ref):
    for start, total in tiles([(which, x_ref[...])], high_ref, low_ref, before_ref):
        store(start, total, out_ref)


def spread_kernel(which, x_ref, high_ref, low_ref, before_ref, out_ref):
    for start, total in tiles([(which, x_ref[...])], high_ref, low_ref, before_ref):
        spread(start, total, out_ref)


def last_kernel(which, scale, x_ref, high_ref, low_ref, before_ref, running_ref, out_ref):
    width = running_ref.shape[1]
    mine = lax.axis_index("xl")
    first = lax.axis_index("y") == 0
    for start, total in tiles([(which, x_ref[...])], high_ref, low_ref, before_ref):
        side, within = divmod(start, width)
        running = running_ref[:, within : within + 256]
        adds = jnp.logical_and(first, mine == side)
        total = total / scale + jnp.where(adds, running, jnp.zeros_like(running))
        for copy in range(8):
            out_ref[copy, :, start : start + 256] = total


def combine_kernel(scale, parts_ref, running_ref, summand_ref, total_ref):
    summand = parts_ref[0]
    for part in range(1, parts_ref.shape[0]):
        summand = summand + parts_ref[part]
    summand = summand / scale
    summand_ref[...] = summand
    total_ref[...] = running_ref[...] + summand


def call(kernel, out, flops, limit, *operands):
    vmem = pl.BlockSpec(memory_space=pltpu.VMEM)
    shapes = jax.tree.map(lambda shape: jax.ShapeDtypeStruct(shape, jnp.float32), out, is_leaf=lambda o: isinstance(o[0], int))
    return pl.pallas_call(
        kernel,
        out_shape=shapes,
        in_specs=[vmem] * len(operands),
        out_specs=jax.tree.map(lambda _: vmem, shapes),
        cost_estimate=pl.CostEstimate(flops=flops, bytes_accessed=4 << 20, transcendentals=0),
        compiler_params=pltpu.CompilerParams(vmem_limit_bytes=limit),
    )(*operands)


def permute(value, moves):
    return lax.ppermute(value, ROW + COL, moves)


def exchange(value):
    return lax.all_to_all(value, COL, 0, 0, tiled=True)


FLOPS, LIMIT = 100_000_000, 4 << 20


def block_product(block, halves, vectors):
    count, width = block.shape
    other = permute(block, partner_moves(1))
    out = ((count, width), (count, width // 2))
    total, running = call(own_block_kernel, out, 2 * FLOPS, LIMIT, block, *halves, vectors)
    return call(other_block_kernel, (8, count, width // 2), 2 * FLOPS, LIMIT, other, *halves, total), running


def product(piece, halves, scale=None, running=None):
    vectors, width = piece.shape
    rows = halves[0].shape[1]
    others = {}
    for which in ARRIVALS:
        others[which] = permute(piece, partner_moves(which))
    total = call(own_kernel, (vectors, rows), FLOPS, LIMIT, piece, *halves)
    for which in ARRIVALS[:2]:
        kernel = functools.partial(next_kernel, which)
        total = call(kernel, (vectors, rows), FLOPS, LIMIT, others[which], *halves, total)
    which = ARRIVALS[2]
    if running is None:
        kernel = functools.partial(spread_kernel, which)
        return call(kernel, (8, vectors, width), FLOPS, LIMIT, others[which], *halves, total)
    kernel = functools.partial(last_kernel, which, scale)
    return call(kernel, (8, vectors, rows), FLOPS, LIMIT, others[which], *halves, total, running)


def local(matrix, vectors):
    block = permute(vectors, owner_moves())
    halves = prepare(matrix)
    block, halves = lax.optimization_barrier((block, halves))
    partial_value, running = block_product(block, halves, vectors)
    parts = exchange(partial_value)
    for degree in range(1, TERMS):
        kernel = functools.partial(combine_kernel, float(degree * STEPS))
        summand, running = call(kernel, (running.shape,) * 2, 1_000_000, 2 << 20, parts, running)
        piece = permute(summand, owner_moves())
        if degree + 1 < TERMS:
            parts = exchange(product(piece, halves))
        else:
            parts = exchange(product(piece, halves, float(TERMS * STEPS), running))
    return functools.reduce(jnp.add, [parts[part] for part in range(8)])


def solution(mesh):
    fine = Mesh(mesh.devices.reshape(tuple(SIZES.values())), tuple(SIZES))
    placed = (P(ROW, COL), P("rep", ROW))
    return jax.shard_map(local, mesh=fine, in_specs=placed, out_specs=P("rep", ROW), check_vma=False)
```

```python
import functools

import jax
import jax.numpy as jnp
from jax import lax
from jax.experimental import pallas as pl
from jax.experimental.pallas import tpu as pltpu
from jax.sharding import Mesh, PartitionSpec as P

TERMS = 6
STEPS = 1

ROW = ("xh", "zh", "zl")
COL = ("xl", "y")
SIZES = {"xh": 2, "zh": 4, "zl": 2, "xl": 2, "y": 4, "rep": 2}
PLACES = [
    (xh, zh, zl, xl, y)
    for xh in range(2)
    for zh in range(4)
    for zl in range(2)
    for xl in range(2)
    for y in range(4)
]
FAR = 2
ARRIVALS = (3, 1, 2)


def index(xh, zh, zl, xl, y):
    return (((xh * 4 + zh) * 2 + zl) * 2 + xl) * 4 + y


def owner_moves():
    def across(zh, y):
        return y if (y - zh) % 2 else (y + FAR) % 4

    return [
        (index(xh, zh, zl, xl, y), index(xl, across(zh, y), zl ^ int(y == zh), xh, zh))
        for xh, zh, zl, xl, y in PLACES
    ]


def partner_moves(which):
    return [
        (index(xh, zh, zl, xl, y), index(xh, zh ^ (which // 2), zl ^ (which % 2), xl, y))
        for xh, zh, zl, xl, y in PLACES
    ]


def held_half(zh):
    swapped = lax.rem(lax.axis_index("y") + FAR, 4) == zh
    return lax.axis_index("zl") ^ swapped.astype(jnp.int32)


def split(value):
    high = value.astype(jnp.bfloat16)
    low = (value - high.astype(jnp.float32)).astype(jnp.bfloat16)
    return high, low


def prepare_kernel(a_ref, high_ref, low_ref, held, sems):
    blocks = held.shape[0]
    width = held.shape[2]
    zh = lax.axis_index("zh")
    own_half, pair_half = held_half(zh), held_half(zh ^ 1)
    own_side = zh & 1

    def copy(block):
        column = pl.multiple_of(block * width, width)
        return pltpu.make_async_copy(a_ref.at[:, pl.ds(column, width)], held.at[block], sems.at[block])

    for block in range(blocks):
        copy(block).start()

    def step(block, carry):
        copy(block).wait()
        high, low = split(held[block].T)
        half, side, part = block // 4, lax.rem(block // 2, 2), lax.rem(block, 2)
        away = side ^ own_side
        first = own_half + away * (pair_half - own_half)
        place = ((half ^ first) + 2 * away) * 2 + part
        rows = pl.ds(pl.multiple_of(place * width, width), width)
        high_ref[rows, :] = high
        low_ref[rows, :] = low
        return carry

    lax.fori_loop(0, blocks, step, 0)


def prepare(matrix):
    rows, columns = matrix.shape
    width = columns // 8
    half = pltpu.VMEM((columns, rows), jnp.bfloat16)
    return pl.pallas_call(
        prepare_kernel,
        out_shape=(half, half),
        in_specs=[pl.BlockSpec(memory_space=pltpu.HBM)],
        out_specs=(pl.BlockSpec(memory_space=pltpu.VMEM),) * 2,
        scratch_shapes=[
            pltpu.VMEM((8, rows, width), jnp.float32),
            pltpu.SemaphoreType.DMA((8,)),
        ],
        cost_estimate=pl.CostEstimate(flops=4_000_000_000, bytes_accessed=8 << 20, transcendentals=0),
        compiler_params=pltpu.CompilerParams(vmem_limit_bytes=24 << 20),
    )(pltpu.with_memory_space_constraint(matrix, pltpu.HBM))


def tiles(pieces, high_ref, low_ref, before_ref=None):
    depth = high_ref.shape[0] // 4
    operands = []
    for quarter, piece in pieces:
        x_high, x_low = split(piece)
        rows = pl.ds(pl.multiple_of(quarter * depth, depth), depth)
        operands.append((rows, x_high, jnp.concatenate([x_high, x_low], axis=0)))
    for start in range(0, high_ref.shape[1], 256):
        columns = slice(start, start + 256)
        total = None
        for rows, x_high, both in operands:
            vectors = x_high.shape[0]
            first = jnp.dot(both, high_ref[rows, columns], preferred_element_type=jnp.float32)
            second = jnp.dot(x_high, low_ref[rows, columns], preferred_element_type=jnp.float32)
            value = first[:vectors] + (first[vectors:] + second)
            total = value if total is None else total + value
        if before_ref is not None:
            total = before_ref[:, columns] + total
        yield start, total


def block_pieces(which, x_ref):
    width = x_ref.shape[1] // 2
    zh = lax.axis_index("zh")
    side = zh & 1
    differs = held_half(zh) ^ held_half(zh ^ 1)
    at = [pl.multiple_of(place * width, width) for place in (side, 1 - side)]
    quarters = (which, 2 + (differs ^ which))
    return [(quarter, x_ref[:, pl.ds(place, width)]) for quarter, place in zip(quarters, at)]


def store(start, total, out_ref):
    out_ref[:, start : start + 256] = total


def spread(start, total, out_ref):
    side, within = divmod(start, out_ref.shape[2])
    for copy in range(4):
        out_ref[copy * 2 + side, :, within : within + 256] = total


def own_block_kernel(x_ref, high_ref, low_ref, vectors_ref, out_ref, running_ref):
    width = running_ref.shape[1]
    running_ref[...] = vectors_ref[:, pl.ds(pl.multiple_of((lax.axis_index("y") & 1) * width, width), width)]
    for start, total in tiles(block_pieces(0, x_ref), high_ref, low_ref):
        store(start, total, out_ref)


def other_block_kernel(x_ref, high_ref, low_ref, before_ref, out_ref):
    for start, total in tiles(block_pieces(1, x_ref), high_ref, low_ref, before_ref):
        spread(start, total, out_ref)


def own_kernel(x_ref, high_ref, low_ref, out_ref):
    for start, total in tiles([(0, x_ref[...])], high_ref, low_ref):
        store(start, total, out_ref)


def next_kernel(which, x_ref, high_ref, low_ref, before_ref, out_ref):
    for start, total in tiles([(which, x_ref[...])], high_ref, low_ref, before_ref):
        store(start, total, out_ref)


def spread_kernel(which, x_ref, high_ref, low_ref, before_ref, out_ref):
    for start, total in tiles([(which, x_ref[...])], high_ref, low_ref, before_ref):
        spread(start, total, out_ref)


def last_kernel(which, scale, x_ref, high_ref, low_ref, before_ref, running_ref, out_ref):
    width = running_ref.shape[1]
    mine = lax.axis_index("y")
    first = lax.axis_index("xl") == 0
    for start, total in tiles([(which, x_ref[...])], high_ref, low_ref, before_ref):
        side, within = divmod(start, width)
        running = running_ref[:, within : within + 256]
        adds = jnp.logical_and(first, mine == side)
        total = total / scale + jnp.where(adds, running, jnp.zeros_like(running))
        for copy in range(8):
            out_ref[copy, :, start : start + 256] = total


def combine_kernel(scale, parts_ref, running_ref, summand_ref, total_ref):
    summand = parts_ref[0]
    for part in range(1, parts_ref.shape[0]):
        summand = summand + parts_ref[part]
    summand = summand / scale
    summand_ref[...] = summand
    total_ref[...] = running_ref[...] + summand


def call(kernel, out, flops, limit, *operands):
    vmem = pl.BlockSpec(memory_space=pltpu.VMEM)
    shapes = jax.tree.map(lambda shape: jax.ShapeDtypeStruct(shape, jnp.float32), out, is_leaf=lambda o: isinstance(o[0], int))
    return pl.pallas_call(
        kernel,
        out_shape=shapes,
        in_specs=[vmem] * len(operands),
        out_specs=jax.tree.map(lambda _: vmem, shapes),
        cost_estimate=pl.CostEstimate(flops=flops, bytes_accessed=4 << 20, transcendentals=0),
        compiler_params=pltpu.CompilerParams(vmem_limit_bytes=limit),
    )(*operands)


def permute(value, moves):
    return lax.ppermute(value, ROW + COL, moves)


def exchange(value):
    return lax.all_to_all(value, COL, 0, 0, tiled=True)


FLOPS, LIMIT = 100_000_000, 4 << 20


def block_product(block, halves, vectors):
    count, width = block.shape
    other = permute(block, partner_moves(1))
    out = ((count, width), (count, width // 2))
    total, running = call(own_block_kernel, out, 2 * FLOPS, LIMIT, block, *halves, vectors)
    return call(other_block_kernel, (8, count, width // 2), 2 * FLOPS, LIMIT, other, *halves, total), running


def product(piece, halves, scale=None, running=None):
    vectors, width = piece.shape
    rows = halves[0].shape[1]
    others = {}
    for which in ARRIVALS:
        others[which] = permute(piece, partner_moves(which))
    total = call(own_kernel, (vectors, rows), FLOPS, LIMIT, piece, *halves)
    for which in ARRIVALS[:2]:
        kernel = functools.partial(next_kernel, which)
        total = call(kernel, (vectors, rows), FLOPS, LIMIT, others[which], *halves, total)
    which = ARRIVALS[2]
    if running is None:
        kernel = functools.partial(spread_kernel, which)
        return call(kernel, (8, vectors, width), FLOPS, LIMIT, others[which], *halves, total)
    kernel = functools.partial(last_kernel, which, scale)
    return call(kernel, (8, vectors, rows), FLOPS, LIMIT, others[which], *halves, total, running)


def local(matrix, vectors):
    block = permute(vectors, owner_moves())
    halves = prepare(matrix)
    block, halves = lax.optimization_barrier((block, halves))
    partial_value, running = block_product(block, halves, vectors)
    parts = exchange(partial_value)
    for degree in range(1, TERMS):
        kernel = functools.partial(combine_kernel, float(degree * STEPS))
        summand, running = call(kernel, (running.shape,) * 2, 1_000_000, 2 << 20, parts, running)
        piece = permute(summand, owner_moves())
        if degree + 1 < TERMS:
            parts = exchange(product(piece, halves))
        else:
            parts = exchange(product(piece, halves, float(TERMS * STEPS), running))
    return functools.reduce(jnp.add, [parts[part] for part in range(8)])


def solution(mesh):
    fine = Mesh(mesh.devices.reshape(tuple(SIZES.values())), tuple(SIZES))
    placed = (P(ROW, COL), P("rep", ROW))
    return jax.shard_map(local, mesh=fine, in_specs=placed, out_specs=P("rep", ROW), check_vma=False)
```

```python
import functools

import jax
import jax.numpy as jnp
from jax import lax
from jax.experimental import pallas as pl
from jax.experimental.pallas import tpu as pltpu
from jax.sharding import Mesh, PartitionSpec as P

TERMS = 6
STEPS = 1

ROW = ("xh", "zh", "zl")
COL = ("xl", "y")
SIZES = {"xh": 2, "zh": 4, "zl": 2, "xl": 2, "y": 4, "rep": 2}
PLACES = [
    (xh, zh, zl, xl, y)
    for xh in range(2)
    for zh in range(4)
    for zl in range(2)
    for xl in range(2)
    for y in range(4)
]
FAR = 2
ARRIVALS = (1, 3, 2)


def index(xh, zh, zl, xl, y):
    return (((xh * 4 + zh) * 2 + zl) * 2 + xl) * 4 + y


def owner_moves():
    def across(zh, y):
        return y if (y - zh) % 2 else (y + FAR) % 4

    return [
        (index(xh, zh, zl, xl, y), index(xl, across(zh, y), zl ^ int(y == zh), xh, zh))
        for xh, zh, zl, xl, y in PLACES
    ]


def partner_moves(which):
    return [
        (index(xh, zh, zl, xl, y), index(xh, zh ^ (which // 2), zl ^ (which % 2), xl, y))
        for xh, zh, zl, xl, y in PLACES
    ]


def held_half(zh):
    swapped = lax.rem(lax.axis_index("y") + FAR, 4) == zh
    return lax.axis_index("zl") ^ swapped.astype(jnp.int32)


def split(value):
    high = value.astype(jnp.bfloat16)
    low = (value - high.astype(jnp.float32)).astype(jnp.bfloat16)
    return high, low


def prepare_kernel(a_ref, high_ref, low_ref, held, sems):
    blocks = held.shape[0]
    width = held.shape[2]
    zh = lax.axis_index("zh")
    own_half, pair_half = held_half(zh), held_half(zh ^ 1)
    own_side = zh & 1

    def copy(block):
        column = pl.multiple_of(block * width, width)
        return pltpu.make_async_copy(a_ref.at[:, pl.ds(column, width)], held.at[block], sems.at[block])

    for block in range(blocks):
        copy(block).start()

    def step(block, carry):
        copy(block).wait()
        high, low = split(held[block].T)
        half, side, part = block // 4, lax.rem(block // 2, 2), lax.rem(block, 2)
        away = side ^ own_side
        first = own_half + away * (pair_half - own_half)
        place = ((half ^ first) + 2 * away) * 2 + part
        rows = pl.ds(pl.multiple_of(place * width, width), width)
        high_ref[rows, :] = high
        low_ref[rows, :] = low
        return carry

    lax.fori_loop(0, blocks, step, 0)


def prepare(matrix):
    rows, columns = matrix.shape
    width = columns // 8
    half = pltpu.VMEM((columns, rows), jnp.bfloat16)
    return pl.pallas_call(
        prepare_kernel,
        out_shape=(half, half),
        in_specs=[pl.BlockSpec(memory_space=pltpu.HBM)],
        out_specs=(pl.BlockSpec(memory_space=pltpu.VMEM),) * 2,
        scratch_shapes=[
            pltpu.VMEM((8, rows, width), jnp.float32),
            pltpu.SemaphoreType.DMA((8,)),
        ],
        cost_estimate=pl.CostEstimate(flops=4_000_000_000, bytes_accessed=8 << 20, transcendentals=0),
        compiler_params=pltpu.CompilerParams(vmem_limit_bytes=24 << 20),
    )(pltpu.with_memory_space_constraint(matrix, pltpu.HBM))


def tiles(pieces, high_ref, low_ref, before_ref=None):
    depth = high_ref.shape[0] // 4
    operands = []
    for quarter, piece in pieces:
        x_high, x_low = split(piece)
        rows = pl.ds(pl.multiple_of(quarter * depth, depth), depth)
        operands.append((rows, x_high, jnp.concatenate([x_high, x_low], axis=0)))
    for start in range(0, high_ref.shape[1], 256):
        columns = slice(start, start + 256)
        total = None
        for rows, x_high, both in operands:
            vectors = x_high.shape[0]
            first = jnp.dot(both, high_ref[rows, columns], preferred_element_type=jnp.float32)
            second = jnp.dot(x_high, low_ref[rows, columns], preferred_element_type=jnp.float32)
            value = first[:vectors] + (first[vectors:] + second)
            total = value if total is None else total + value
        if before_ref is not None:
            total = before_ref[:, columns] + total
        yield start, total


def block_pieces(which, x_ref):
    width = x_ref.shape[1] // 2
    zh = lax.axis_index("zh")
    side = zh & 1
    differs = held_half(zh) ^ held_half(zh ^ 1)
    at = [pl.multiple_of(place * width, width) for place in (side, 1 - side)]
    quarters = (which, 2 + (differs ^ which))
    return [(quarter, x_ref[:, pl.ds(place, width)]) for quarter, place in zip(quarters, at)]


def store(start, total, out_ref):
    out_ref[:, start : start + 256] = total


def spread(start, total, out_ref):
    side, within = divmod(start, out_ref.shape[2])
    for copy in range(4):
        out_ref[copy * 2 + side, :, within : within + 256] = total


def own_block_kernel(x_ref, high_ref, low_ref, vectors_ref, out_ref, running_ref):
    width = running_ref.shape[1]
    running_ref[...] = vectors_ref[:, pl.ds(pl.multiple_of((lax.axis_index("y") & 1) * width, width), width)]
    for start, total in tiles(block_pieces(0, x_ref), high_ref, low_ref):
        store(start, total, out_ref)


def other_block_kernel(x_ref, high_ref, low_ref, before_ref, out_ref):
    for start, total in tiles(block_pieces(1, x_ref), high_ref, low_ref, before_ref):
        spread(start, total, out_ref)


def own_kernel(x_ref, high_ref, low_ref, out_ref):
    for start, total in tiles([(0, x_ref[...])], high_ref, low_ref):
        store(start, total, out_ref)


def two_kernel(x_ref, y_ref, high_ref, low_ref, before_ref, out_ref):
    pieces = [(which, ref[...]) for which, ref in zip(ARRIVALS, (x_ref, y_ref))]
    for start, total in tiles(pieces, high_ref, low_ref, before_ref):
        store(start, total, out_ref)


def spread_kernel(which, x_ref, high_ref, low_ref, before_ref, out_ref):
    for start, total in tiles([(which, x_ref[...])], high_ref, low_ref, before_ref):
        spread(start, total, out_ref)


def last_kernel(which, scale, x_ref, high_ref, low_ref, before_ref, running_ref, out_ref):
    width = running_ref.shape[1]
    mine = lax.axis_index("y")
    first = lax.axis_index("xl") == 0
    for start, total in tiles([(which, x_ref[...])], high_ref, low_ref, before_ref):
        side, within = divmod(start, width)
        running = running_ref[:, within : within + 256]
        adds = jnp.logical_and(first, mine == side)
        total = total / scale + jnp.where(adds, running, jnp.zeros_like(running))
        for copy in range(8):
            out_ref[copy, :, start : start + 256] = total


def combine_kernel(scale, parts_ref, running_ref, summand_ref, total_ref):
    summand = parts_ref[0]
    for part in range(1, parts_ref.shape[0]):
        summand = summand + parts_ref[part]
    summand = summand / scale
    summand_ref[...] = summand
    total_ref[...] = running_ref[...] + summand


def call(kernel, out, flops, limit, *operands):
    vmem = pl.BlockSpec(memory_space=pltpu.VMEM)
    shapes = jax.tree.map(lambda shape: jax.ShapeDtypeStruct(shape, jnp.float32), out, is_leaf=lambda o: isinstance(o[0], int))
    return pl.pallas_call(
        kernel,
        out_shape=shapes,
        in_specs=[vmem] * len(operands),
        out_specs=jax.tree.map(lambda _: vmem, shapes),
        cost_estimate=pl.CostEstimate(flops=flops, bytes_accessed=4 << 20, transcendentals=0),
        compiler_params=pltpu.CompilerParams(vmem_limit_bytes=limit),
    )(*operands)


def permute(value, moves):
    return lax.ppermute(value, ROW + COL, moves)


def exchange(value):
    return lax.all_to_all(value, COL, 0, 0, tiled=True)


FLOPS, LIMIT = 100_000_000, 4 << 20


def block_product(block, halves, vectors):
    count, width = block.shape
    other = permute(block, partner_moves(1))
    out = ((count, width), (count, width // 2))
    total, running = call(own_block_kernel, out, 2 * FLOPS, LIMIT, block, *halves, vectors)
    return call(other_block_kernel, (8, count, width // 2), 2 * FLOPS, LIMIT, other, *halves, total), running


def product(piece, halves, scale=None, running=None):
    vectors, width = piece.shape
    rows = halves[0].shape[1]
    others = {}
    for which in ARRIVALS:
        others[which] = permute(piece, partner_moves(which))
    total = call(own_kernel, (vectors, rows), FLOPS, LIMIT, piece, *halves)
    arrived = [others[which] for which in ARRIVALS[:2]]
    total = call(two_kernel, (vectors, rows), 2 * FLOPS, LIMIT, *arrived, *halves, total)
    which = ARRIVALS[2]
    if running is None:
        kernel = functools.partial(spread_kernel, which)
        return call(kernel, (8, vectors, width), FLOPS, LIMIT, others[which], *halves, total)
    kernel = functools.partial(last_kernel, which, scale)
    return call(kernel, (8, vectors, rows), FLOPS, LIMIT, others[which], *halves, total, running)


def local(matrix, vectors):
    block = permute(vectors, owner_moves())
    halves = prepare(matrix)
    block, halves = lax.optimization_barrier((block, halves))
    partial_value, running = block_product(block, halves, vectors)
    parts = exchange(partial_value)
    for degree in range(1, TERMS):
        kernel = functools.partial(combine_kernel, float(degree * STEPS))
        summand, running = call(kernel, (running.shape,) * 2, 1_000_000, 2 << 20, parts, running)
        piece = permute(summand, owner_moves())
        if degree + 1 < TERMS:
            parts = exchange(product(piece, halves))
        else:
            parts = exchange(product(piece, halves, float(TERMS * STEPS), running))
    return functools.reduce(jnp.add, [parts[part] for part in range(8)])


def solution(mesh):
    fine = Mesh(mesh.devices.reshape(tuple(SIZES.values())), tuple(SIZES))
    placed = (P(ROW, COL), P("rep", ROW))
    return jax.shard_map(local, mesh=fine, in_specs=placed, out_specs=P("rep", ROW), check_vma=False)
```
